32 devices in a mesh: dp: 8 (over y, x, core), tensor: 4 (over z).
Axes of the slice: x: 2, y: 2, z: 4, core: 2. Of those that a mesh axis runs over, the one named last changes fastest.
Arguments:
- tokens: bfloat16 [128, 196, 768], P(('dp', 'tensor')), may hold values from -6 to 6
- space_gain: float32 [768], replicated, may hold values from 0.5 to 1.5
- space_shift: float32 [768], replicated, may hold values from -3 to 3
- space_inproj: bfloat16 [768, 3, 768], P(None, None, 'tensor'), may hold values from -0.21875 to 0.21875
- space_bias: bfloat16 [2, 768], P(None, 'tensor'), may hold values from -3 to 3
- space_outproj: bfloat16 [768, 768], P('tensor'), may hold values from -1.75 to 1.75
- space_outbias: bfloat16 [768], replicated, may hold values from -3 to 3
- time_gain: float32 [768], replicated, may hold values from 0.5 to 1.5
- time_shift: float32 [768], replicated, may hold values from -3 to 3
- time_inproj: bfloat16 [768, 3, 768], P(None, None, 'tensor'), may hold values from -0.21875 to 0.21875
- time_bias: bfloat16 [2, 768], P(None, 'tensor'), may hold values from -3 to 3
- time_outproj: bfloat16 [768, 768], P('tensor'), may hold values from -0.5 to 0.5
- time_outbias: bfloat16 [768], replicated, may hold values from -3 to 3
- feed_gain: float32 [768], replicated, may hold values from 0.5 to 1.5
- feed_shift: float32 [768], replicated, may hold values from -3 to 3
- up_weight: bfloat16 [3072, 768], P('tensor'), may hold values from -0.21875 to 0.21875
- up_bias: bfloat16 [3072], P('tensor'), may hold values from -3 to 3
- down_weight: bfloat16 [3072, 768], P('tensor'), may hold values from -0.15625 to 0.15625
- down_bias: bfloat16 [768], replicated, may hold values from -3 to 3
- cotangent: bfloat16 [128, 196, 768], P(('dp', 'tensor')), may hold values from -6 to 6
Outputs:
- layer_out: bfloat16 [128, 196, 768], P(('dp', 'tensor'))
- input_gradient: float32 [128, 196, 768], P(('dp', 'tensor'))
- space_gain_gradient: float32 [768], replicated
- space_shift_gradient: float32 [768], replicated
- space_inproj_gradient: float32 [768, 3, 768], P(None, None, 'tensor')
- space_bias_gradient: float32 [2, 768], P(None, 'tensor')
- space_outproj_gradient: float32 [768, 768], P('tensor')
- space_outbias_gradient: float32 [768], replicated
- time_gain_gradient: float32 [768], replicated
- time_shift_gradient: float32 [768], replicated
- time_inproj_gradient: float32 [768, 3, 768], P(None, None, 'tensor')
- time_bias_gradient: float32 [2, 768], P(None, 'tensor')
- time_outproj_gradient: float32 [768, 768], P('tensor')
- time_outbias_gradient: float32 [768], replicated
- feed_gain_gradient: float32 [768], replicated
- feed_shift_gradient: float32 [768], replicated
- up_weight_gradient: float32 [3072, 768], P('tensor')
- up_bias_gradient: float32 [3072], P('tensor')
- down_weight_gradient: float32 [3072, 768], P('tensor')
- down_bias_gradient: float32 [768], replicated
The draws below stay inside these ranges and needn't reach their ends.
All inputs are finite; a program needn't handle non-finite values.
Results may differ from the reference program's by a relative error of at most 0.013.
The reference program's roundings to bfloat16 on the way count: a program that leaves them out, or rounds other values in their place, can miss the bound.
Values may be sent and summed in bfloat16 or wider, within the bound.
A program may use at most 192 MiB of HBM per device.

```python
import jax
import jax.numpy as jnp
from jax import lax

D = 768
NH = 12
HS = 64
FF = 3072
PATCH = 196
TIMES = 16
CLIPS = 8
FRAMES = 128


def shard_levels(key, shape, pieces, least, high):
    level = 1.0
    for dim, shards_of in pieces:
        draws = jax.random.uniform(jax.random.fold_in(jax.random.fold_in(key, 6), dim), (shards_of,), jnp.float32, least / len(pieces), high / len(pieces))
        level = level * jnp.repeat(jnp.exp(draws), shape[dim] // shards_of).reshape((-1,) + (1,) * (len(shape) - 1 - dim))
    return level


def gaussian(stream_key, extent, width, reach, shards=(), held_as=jnp.bfloat16):
    level = shard_levels(stream_key, extent, shards, -0.22, 0.18) if shards else 1.0
    result = jax.random.normal(stream_key, extent, jnp.float32) * width * level
    return jnp.minimum(jnp.maximum(result, -reach), reach).astype(held_as)


def setup_inputs(seed: int = 0) -> dict:
    key_list = jax.random.split(jax.random.key(seed), 21)
    tokens = gaussian(key_list[0], (FRAMES, PATCH, D), 1.0, 6.0, ((0, 32),))
    space_gain = jnp.clip(1.0 + 0.1 * jax.random.normal(key_list[1], (D,), jnp.float32), 0.5, 1.5)
    space_shift = gaussian(key_list[2], (D,), 0.5, 3.0, (), jnp.float32)
    space_inproj = gaussian(key_list[3], (D, 3, D), D ** -0.5, 0.21875, ((2, 4),))
    space_bias = gaussian(key_list[4], (2, D), 0.5, 3.0, ((1, 4),))
    space_outproj = gaussian(key_list[5], (D, D), (D * 3 // PATCH) ** -0.5, 1.75, ((0, 4),))
    space_outbias = gaussian(key_list[6], (D,), 0.5, 3.0)
    time_gain = jnp.clip(1.0 + 0.1 * jax.random.normal(key_list[7], (D,), jnp.float32), 0.5, 1.5)
    time_shift = gaussian(key_list[8], (D,), 0.5, 3.0, (), jnp.float32)
    time_inproj = gaussian(key_list[9], (D, 3, D), D ** -0.5, 0.21875, ((2, 4),))
    time_bias = gaussian(key_list[10], (2, D), 0.5, 3.0, ((1, 4),))
    time_outproj = gaussian(key_list[11], (D, D), (D * 3 // TIMES) ** -0.5, 0.5, ((0, 4),))
    time_outbias = gaussian(key_list[12], (D,), 0.5, 3.0)
    feed_gain = jnp.clip(1.0 + 0.1 * jax.random.normal(key_list[13], (D,), jnp.float32), 0.5, 1.5)
    feed_shift = gaussian(key_list[14], (D,), 0.5, 3.0, (), jnp.float32)
    up_weight = gaussian(key_list[15], (FF, D), D ** -0.5, 0.21875, ((0, 4),))
    up_bias = gaussian(key_list[16], (FF,), 0.5, 3.0, ((0, 4),))
    down_weight = gaussian(key_list[17], (FF, D), (FF // 2) ** -0.5, 0.15625, ((0, 4),))
    down_bias = gaussian(key_list[18], (D,), 0.5, 3.0)
    cotangent = gaussian(key_list[19], (FRAMES, PATCH, D), 1.0, 6.0, ((0, 32),))
    return dict(tokens=tokens, space_gain=space_gain, space_shift=space_shift, space_inproj=space_inproj, space_bias=space_bias, space_outproj=space_outproj, space_outbias=space_outbias, time_gain=time_gain, time_shift=time_shift, time_inproj=time_inproj, time_bias=time_bias, time_outproj=time_outproj, time_outbias=time_outbias, feed_gain=feed_gain, feed_shift=feed_shift, up_weight=up_weight, up_bias=up_bias, down_weight=down_weight, down_bias=down_bias, cotangent=cotangent)


@jax.custom_vjp
def low(v):
    return lax.optimization_barrier(v.astype(jnp.bfloat16)).astype(jnp.float32)

@jax.custom_vjp
def low_back(v):
    return v

def low_keep(v):
    return (low(v), None)

def low_pass(kept, grad):
    return (grad,)

def back_keep(v):
    return (v, None)

def back_low(kept, grad):
    return (low(grad),)
low.defvjp(low_keep, low_pass)
low_back.defvjp(back_keep, back_low)
EPSILON = 1e-06
ROOT_HALF = 0.7071067811865476
HIGHEST = lax.Precision.HIGHEST

def layer_norm(values, gain, shift):
    center = values - lax.optimization_barrier(jnp.mean(values, axis=-1, keepdims=True))
    second = lax.optimization_barrier(jnp.mean(center * center, axis=-1, keepdims=True))
    return center * lax.rsqrt(second + EPSILON) * gain + shift

def gelu_exact(values):
    return 0.5 * values * (1.0 + lax.erf(values * ROOT_HALF))

def attend(queries, keys, values):
    qk_scale = HS ** (-0.5)
    scores = low_back(jnp.einsum('blhe,bmhe->bhlm', queries, keys, precision=HIGHEST) * qk_scale)
    probs = low(jax.nn.softmax(scores, axis=-1))
    return jnp.einsum('bhlm,bmhe->blhe', probs, values, precision=HIGHEST)

def attend_group(group):
    return attend(group[0], group[1], group[2])

def attend_blocks(queries, keys, values):
    return lax.map(jax.checkpoint(attend_group), (queries, keys, values))

def attention_block(resid, gain, shift, inproj, bias_pair, outproj, outbias, temporal):
    normed = low(layer_norm(resid, gain, shift))
    zero_row = jnp.zeros((1, D), jnp.float32)
    bias = jnp.concatenate([bias_pair[0:1], zero_row, bias_pair[1:2]], axis=0).reshape(3 * D)
    projected = jnp.einsum('tcpd,de->tcpe', normed, inproj.reshape(D, 3 * D), precision=HIGHEST) + bias
    projected = low_back(low(projected)).reshape(TIMES, CLIPS, PATCH, 3, NH, HS)
    queries = projected[:, :, :, 0]
    keys = projected[:, :, :, 1]
    values = projected[:, :, :, 2]
    if temporal:
        order = (1, 2, 0, 3, 4)
        mixed = attend_blocks(queries.transpose(order), keys.transpose(order), values.transpose(order))
        mixed = mixed.transpose(2, 0, 1, 3, 4)
    else:
        shape = (-1, TIMES, PATCH, NH, HS)
        mixed = attend_blocks(queries.reshape(shape), keys.reshape(shape), values.reshape(shape))
        mixed = mixed.reshape(TIMES, CLIPS, PATCH, NH, HS)
    mixed = low_back(low(mixed.reshape(TIMES, CLIPS, PATCH, D)))
    branch = jnp.einsum('tcpd,de->tcpe', mixed, outproj, precision=HIGHEST) + outbias
    return resid + low_back(branch)

def feed_block(resid, gain, shift, up_weight, up_bias, down_weight, down_bias):
    normed = low(layer_norm(resid, gain, shift))
    pre_act = low_back(jnp.einsum('tcpd,fd->tcpf', normed, up_weight, precision=HIGHEST) + up_bias)
    hidden = low(gelu_exact(pre_act))
    branch = jnp.einsum('tcpf,fd->tcpd', hidden, down_weight, precision=HIGHEST) + down_bias
    return resid + low_back(branch)

def forward(tokens, space_gain, space_shift, space_inproj, space_bias, space_outproj, space_outbias, time_gain, time_shift, time_inproj, time_bias, time_outproj, time_outbias, feed_gain, feed_shift, up_weight, up_bias, down_weight, down_bias):
    resid = tokens.reshape(TIMES, CLIPS, PATCH, D)
    resid = attention_block(resid, space_gain, space_shift, space_inproj, space_bias, space_outproj, space_outbias, False)
    resid = attention_block(resid, time_gain, time_shift, time_inproj, time_bias, time_outproj, time_outbias, True)
    resid = feed_block(resid, feed_gain, feed_shift, up_weight, up_bias, down_weight, down_bias)
    return resid.reshape(FRAMES, PATCH, D)

def reference(tokens, space_gain, space_shift, space_inproj, space_bias, space_outproj, space_outbias, time_gain, time_shift, time_inproj, time_bias, time_outproj, time_outbias, feed_gain, feed_shift, up_weight, up_bias, down_weight, down_bias, cotangent):
    inputs = (tokens, space_gain, space_shift, space_inproj, space_bias, space_outproj, space_outbias, time_gain, time_shift, time_inproj, time_bias, time_outproj, time_outbias, feed_gain, feed_shift, up_weight, up_bias, down_weight, down_bias)
    primals = tuple((item.astype(jnp.float32) for item in inputs))
    layer_sum, pullback = jax.vjp(forward, *primals)
    grads = pullback(cotangent.astype(jnp.float32))
    return (layer_sum.astype(jnp.bfloat16), grads[0], grads[1], grads[2], grads[3], grads[4], grads[5], grads[6], grads[7], grads[8], grads[9], grads[10], grads[11], grads[12], grads[13], grads[14], grads[15], grads[16], grads[17], grads[18])
```

```python
import jax
import jax.numpy as jnp
from jax import lax
from jax.sharding import Mesh, PartitionSpec as P

HS = 64
PATCH = 196
TIMES = 16
EPSILON = 1e-06
ROOT_HALF = 0.7071067811865476
INV_ROOT_TAU = 0.3989422804014327
F32 = jnp.float32
BF16 = jnp.bfloat16
NT = (((1,), (1,)), ((), ()))
NN = (((1,), (0,)), ((), ()))
TN = (((0,), (0,)), ((), ()))


def dot(a, b, dims):
    return lax.dot_general(a, b, dims, preferred_element_type=F32)


def norm_stats(values):
    center = values - jnp.mean(values, axis=-1, keepdims=True)
    second = jnp.mean(center * center, axis=-1, keepdims=True)
    rate = lax.rsqrt(second + EPSILON)
    return center * rate, rate


def norm_back(grad, normed, rate, gain):
    e = grad * gain
    inner = jnp.mean(e * normed, axis=-1, keepdims=True)
    return rate * (e - jnp.mean(e, axis=-1, keepdims=True) - normed * inner)


def gelu_exact(values):
    return 0.5 * values * (1.0 + lax.erf(values * ROOT_HALF))


def gelu_slope(values):
    return (
        0.5 * (1.0 + lax.erf(values * ROOT_HALF))
        + values * jnp.exp(-0.5 * values * values) * INV_ROOT_TAU
    )


def forms(batch_first):
    if batch_first:
        return ("blhe", "bmhe", "bhlm")
    return ("lbhe", "mbhe", "bhlm")


def esum(form, a, b):
    return jnp.einsum(form, a, b, preferred_element_type=F32)


def attend(queries, keys, values, batch_first):
    q, k, s = forms(batch_first)
    scores = esum(q + "," + k + "->" + s, queries, keys) * (HS ** -0.5)
    top = jnp.max(scores, axis=-1, keepdims=True)
    weights = jnp.exp(scores - top)
    total = jnp.sum(weights, axis=-1, keepdims=True)
    probs = (weights / total).astype(BF16)
    return esum(s + "," + k + "->" + q, probs, values), top + jnp.log(total)


def attend_back(queries, keys, values, log_total, mixed_grad, batch_first):
    q, k, s = forms(batch_first)
    scale = HS ** -0.5
    scores = esum(q + "," + k + "->" + s, queries, keys) * scale
    probs = jnp.exp(scores - log_total)
    value_grad = esum(s + "," + q + "->" + k, probs.astype(BF16), mixed_grad)
    prob_grad = esum(q + "," + k + "->" + s, mixed_grad, values)
    inner = jnp.sum(prob_grad * probs, axis=-1, keepdims=True)
    score_grad = (probs * (prob_grad - inner)).astype(BF16)
    query_grad = esum(s + "," + k + "->" + q, score_grad, keys) * scale
    key_grad = esum(s + "," + q + "->" + k, score_grad, queries) * scale
    return query_grad, key_grad, value_grad


def build(mesh):
    dp, tp = mesh.shape["dp"], mesh.shape["tensor"]
    count = dp * tp
    groups = count // TIMES
    if groups <= tp:
        shape = (dp, tp // groups, groups)
        names = dict(time=("a", "b"), tensor=("b", "c"), dp=("a",))
    else:
        shape = (TIMES, groups // tp, tp)
        names = dict(time=("a",), tensor=("c",), dp=("a", "b"))
    inner = Mesh(mesh.devices.reshape(shape), ("a", "b", "c"))
    return inner, names, dp, tp


def make_device(names, dp, tp):
    every = ("a", "b", "c")

    def regroup(x):
        return lax.all_to_all(x, names["time"], split_axis=0, concat_axis=0, tiled=True)

    def gather_all(piece):
        full = lax.all_gather(piece, every, axis=0, tiled=False)
        return full.reshape((dp, tp) + piece.shape)

    def per_device(
        tokens, space_gain, space_shift, space_inproj, space_bias, space_outproj,
        space_outbias, time_gain, time_shift, time_inproj, time_bias, time_outproj,
        time_outbias, feed_gain, feed_shift, up_weight, up_bias, down_weight,
        down_bias, cotangent,
    ):
        width = tokens.shape[-1]
        own = tokens.shape[0] * tokens.shape[1]
        heads_width = space_inproj.shape[2]
        heads = tp * heads_width // HS
        units = up_weight.shape[0]
        d_index = lax.axis_index(names["dp"])
        k_index = lax.axis_index(names["tensor"])
        hp, up = heads_width // dp, units // dp

        def piece_of(rows, per):
            return lax.dynamic_slice_in_dim(rows, d_index * per, per, rows.ndim - 2)

        def attn_piece(inproj, outproj):
            in_piece = piece_of(inproj.transpose(1, 2, 0), hp).reshape(3 * hp, width)
            return jnp.concatenate([in_piece, piece_of(outproj, hp)], axis=0)

        def attn_full(full):
            w_in = full[:, :, : 3 * hp].reshape(dp, tp, 3, hp, width)
            w_in = w_in.transpose(2, 1, 0, 3, 4).reshape(3 * width, width)
            w_out = full[:, :, 3 * hp : 4 * hp].transpose(1, 0, 2, 3).reshape(width, width)
            return w_in, w_out

        bias_piece = jnp.concatenate(
            [
                lax.dynamic_slice_in_dim(up_bias, d_index * up, up, 0),
                lax.dynamic_slice_in_dim(space_bias, d_index * hp, hp, 1).reshape(-1),
                lax.dynamic_slice_in_dim(time_bias, d_index * hp, hp, 1).reshape(-1),
            ]
        )
        bias_row = jnp.zeros((8, width), BF16).at[0, : bias_piece.shape[0]].set(bias_piece)
        full_space = gather_all(
            jnp.concatenate([attn_piece(space_inproj, space_outproj), bias_row], axis=0)
        )
        full_time = gather_all(attn_piece(time_inproj, time_outproj))
        full_feed = gather_all(
            jnp.concatenate([piece_of(up_weight, up), piece_of(down_weight, up)], axis=0)
        )
        space_in_w, space_out_w = attn_full(full_space)
        time_in_w, time_out_w = attn_full(full_time)
        up_w = full_feed[:, :, :up].reshape(dp * tp * up, width)
        down_w = full_feed[:, :, up:].reshape(dp * tp * up, width)
        bias_all = full_space[:, :, 4 * hp].astype(F32)
        up_b = bias_all[:, :, :up].reshape(-1)

        def in_bias(start):
            pair = bias_all[:, :, start : start + 2 * hp].reshape(dp, tp, 2, hp)
            pair = pair.transpose(2, 1, 0, 3).reshape(2, width)
            return jnp.concatenate([pair[0], jnp.zeros((width,), F32), pair[1]])

        space_b, time_b = in_bias(up), in_bias(up + 2 * hp)

        cot = regroup(cotangent.reshape(TIMES, own // TIMES, width)).reshape(own, width)

        resid = tokens.reshape(own, width).astype(F32)
        space_n, space_r = norm_stats(resid)
        space_in = (space_n * space_gain + space_shift).astype(BF16)
        space_qkv = (dot(space_in, space_in_w, NT) + space_b).astype(BF16)
        split = space_qkv.reshape(-1, PATCH, 3, heads, HS)
        mixed, space_log = attend(split[:, :, 0], split[:, :, 1], split[:, :, 2], True)
        space_mix = mixed.astype(BF16).reshape(own, width)
        after_space = resid + dot(space_mix, space_out_w, NN) + space_outbias.astype(F32)
        tn, _ = norm_stats(after_space)
        time_in_own = (tn * time_gain + time_shift).astype(BF16)

        time_in = regroup(time_in_own.reshape(TIMES, own // TIMES, width)).reshape(own, width)
        after_space_p = regroup(after_space.reshape(TIMES, own // TIMES, width)).reshape(own, width)
        time_qkv = (dot(time_in, time_in_w, NT) + time_b).astype(BF16)
        tsplit = time_qkv.reshape(TIMES, -1, 3, heads, HS)
        tmixed, time_log = attend(tsplit[:, :, 0], tsplit[:, :, 1], tsplit[:, :, 2], False)
        time_mix = tmixed.astype(BF16).reshape(own, width)
        after_time = after_space_p + dot(time_mix, time_out_w, NN) + time_outbias.astype(F32)
        feed_n, feed_r = norm_stats(after_time)
        feed_in = (feed_n * feed_gain + feed_shift).astype(BF16)
        pre = dot(feed_in, up_w, NT) + up_b
        hidden = gelu_exact(pre).astype(BF16)
        layer_p = (after_time + dot(hidden, down_w, NN) + down_bias.astype(F32)).astype(BF16)
        layer_out = regroup(layer_p.reshape(TIMES, -1, width)).reshape(tokens.shape)

        upstream = cot.astype(F32)
        down_bias_g = jnp.sum(upstream, axis=0)
        down_g = dot(hidden, cot, TN)
        pre_g = (dot(cot, down_w, NT) * gelu_slope(pre)).astype(BF16)
        up_g = dot(pre_g, feed_in, TN)
        up_bias_g = jnp.sum(pre_g.astype(F32), axis=0)
        feed_g = dot(pre_g, up_w, NN)
        feed_gain_g = jnp.sum(feed_g * feed_n, axis=0)
        feed_shift_g = jnp.sum(feed_g, axis=0)
        after_time_g = upstream + norm_back(feed_g, feed_n, feed_r, feed_gain)

        def scatter(grad):
            return lax.psum_scatter(
                grad.astype(BF16), every, scatter_dimension=0, tiled=False
            )

        feed_pack = jnp.concatenate(
            [up_g.reshape(dp * tp, up, width), down_g.reshape(dp * tp, up, width)], axis=1
        )
        feed_part = scatter(feed_pack)

        def attention_back(upstream, normed_in, qkv, log_total, mix, w_in, w_out, temporal, shape):
            branch = upstream.astype(BF16)
            outbias_g = jnp.sum(branch.astype(F32), axis=0)
            out_g = dot(mix, branch, TN)
            mix_g = dot(branch, w_out, NT).astype(BF16)
            parts = qkv.reshape(shape + (3, heads, HS))
            qg, kg, vg = attend_back(
                parts[:, :, 0], parts[:, :, 1], parts[:, :, 2], log_total,
                mix_g.reshape(shape + (heads, HS)), not temporal,
            )
            qkv_g = jnp.stack([qg, kg, vg], axis=2).astype(BF16).reshape(own, 3 * width)
            sums = jnp.sum(qkv_g.astype(F32), axis=0).reshape(3, width)
            in_g = dot(qkv_g, normed_in, TN)
            normed_g = dot(qkv_g, w_in, NN)
            pack = jnp.concatenate(
                [
                    in_g.reshape(3, tp, dp, hp, width)
                    .transpose(2, 1, 0, 3, 4)
                    .reshape(dp * tp, 3 * hp, width),
                    out_g.reshape(tp, dp, hp, width)
                    .transpose(1, 0, 2, 3)
                    .reshape(dp * tp, hp, width),
                ],
                axis=1,
            )
            return normed_g, pack, outbias_g, sums

        seqs = own // TIMES
        time_in_g, time_pack, time_outbias_g, time_sums = attention_back(
            after_time_g, time_in, time_qkv, time_log, time_mix, time_in_w, time_out_w,
            True, (TIMES, seqs),
        )
        time_part = scatter(time_pack)
        tn_p, tr_p = norm_stats(after_space_p)
        time_gain_g = jnp.sum(time_in_g * tn_p, axis=0)
        time_shift_g = jnp.sum(time_in_g, axis=0)
        after_space_g_p = after_time_g + norm_back(time_in_g, tn_p, tr_p, time_gain)

        high_p = after_space_g_p.astype(BF16)
        low_p = (after_space_g_p - high_p.astype(F32)).astype(BF16)
        high = regroup(high_p.reshape(TIMES, seqs, width)).reshape(own, width)
        low = regroup(low_p.reshape(TIMES, seqs, width)).reshape(own, width)
        after_space_g = high.astype(F32) + low.astype(F32)

        space_in_g, space_pack, space_outbias_g, space_sums = attention_back(
            high, space_in, space_qkv, space_log, space_mix, space_in_w, space_out_w,
            False, (own // PATCH, PATCH),
        )
        space_part = scatter(space_pack)
        space_gain_g = jnp.sum(space_in_g * space_n, axis=0)
        space_shift_g = jnp.sum(space_in_g, axis=0)
        input_g = after_space_g + norm_back(space_in_g, space_n, space_r, space_gain)

        small = jnp.concatenate(
            [
                space_gain_g, space_shift_g, space_outbias_g, time_gain_g, time_shift_g,
                time_outbias_g, feed_gain_g, feed_shift_g, down_bias_g,
                space_sums[0], space_sums[2], time_sums[0], time_sums[2],
                up_bias_g.reshape(dp, tp, up).transpose(1, 0, 2).reshape(-1),
            ]
        )
        small = lax.psum(small, every)
        rows = small[: 13 * width].reshape(13, width)
        head_rows = lax.dynamic_slice_in_dim(rows[9:], k_index * heads_width, heads_width, 1)
        up_bias_out = lax.dynamic_slice_in_dim(small[13 * width :], k_index * units, units, 0)

        def spread(part):
            return lax.all_gather(part, names["dp"], axis=0, tiled=False)

        def attn_out(full):
            in_out = full[:, : 3 * hp].reshape(dp, 3, hp, width).transpose(1, 0, 2, 3)
            in_out = in_out.reshape(3, heads_width, width).transpose(2, 0, 1).astype(F32)
            return in_out, full[:, 3 * hp :].reshape(heads_width, width).astype(F32)

        feed_all = spread(feed_part)
        time_in_out, time_out_out = attn_out(spread(time_part))
        space_in_out, space_out_out = attn_out(spread(space_part))
        return (
            layer_out,
            input_g.reshape(tokens.shape),
            rows[0], rows[1], space_in_out, head_rows[0:2], space_out_out, rows[2],
            rows[3], rows[4], time_in_out, head_rows[2:4], time_out_out, rows[5],
            rows[6], rows[7],
            feed_all[:, :up].reshape(units, width).astype(F32),
            up_bias_out,
            feed_all[:, up:].reshape(units, width).astype(F32),
            rows[8],
        )

    return per_device


def solution(mesh):
    inner, names, dp, tp = build(mesh)
    every, tensor = ("a", "b", "c"), names["tensor"]
    frames = P(every, None, None)
    head_in = P(None, None, tensor)
    head_bias = P(None, tensor)
    row = P(tensor, None)
    return jax.shard_map(
        make_device(names, dp, tp),
        mesh=inner,
        in_specs=(
            frames, P(), P(), head_in, head_bias, row, P(),
            P(), P(), head_in, head_bias, row, P(),
            P(), P(), row, P(tensor), row, P(), frames,
        ),
        out_specs=(
            frames, frames, P(), P(), head_in, head_bias, row, P(),
            P(), P(), head_in, head_bias, row, P(),
            P(), P(), row, P(tensor), row, P(),
        ),
        check_vma=False,
    )
```

```python
import functools

import jax
import jax.numpy as jnp
from jax import lax
from jax.experimental import pallas as pl
from jax.experimental.pallas import tpu as pltpu
from jax.sharding import Mesh, PartitionSpec as P

HS = 64
PATCH = 196
TIMES = 16
SLOT = 56
EPSILON = 1e-06
ROOT_HALF = 0.7071067811865476
INV_ROOT_TAU = 0.3989422804014327
F32 = jnp.float32
BF16 = jnp.bfloat16
NT = (((1,), (1,)), ((), ()))
NN = (((1,), (0,)), ((), ()))
TN = (((0,), (0,)), ((), ()))


def dot(a, b, dims):
    return lax.dot_general(a, b, dims, preferred_element_type=F32)


def norm_stats(values):
    center = values - jnp.mean(values, axis=-1, keepdims=True)
    second = jnp.mean(center * center, axis=-1, keepdims=True)
    rate = lax.rsqrt(second + EPSILON)
    return center * rate, rate


def norm_back(grad, normed, rate, gain):
    e = grad * gain
    inner = jnp.mean(e * normed, axis=-1, keepdims=True)
    return rate * (e - jnp.mean(e, axis=-1, keepdims=True) - normed * inner)


def gelu_exact(values):
    return 0.5 * values * (1.0 + lax.erf(values * ROOT_HALF))


def gelu_slope(values):
    return (
        0.5 * (1.0 + lax.erf(values * ROOT_HALF))
        + values * jnp.exp(-0.5 * values * values) * INV_ROOT_TAU
    )


def same_sequence(rows, temporal):
    r = lax.broadcasted_iota(jnp.int32, (rows, rows), 0)
    c = lax.broadcasted_iota(jnp.int32, (rows, rows), 1)
    if temporal:
        return (r % 8) == (c % 8)
    return (c % SLOT) < (PATCH // 4)


def head_lanes(rows, second):
    lane = lax.broadcasted_iota(jnp.int32, (rows, 2 * HS), 1)
    return (lane >= HS) if second else (lane < HS)


def softmax_of(q_one, k_pair, allowed):
    scores = dot(q_one, k_pair, NT) * (HS ** -0.5)
    scores = jnp.where(allowed, scores, -1e30)
    top = jnp.max(scores, axis=-1, keepdims=True)
    weights = jnp.exp(scores - top)
    return weights / jnp.sum(weights, axis=-1, keepdims=True)


def rows_of(ref, start, temporal):
    if temporal:
        block = ref[:, :, start : start + 2 * HS].astype(F32)
        return block.reshape(-1, 2 * HS).astype(BF16)
    return ref[:, start : start + 2 * HS]


def put_rows(ref, start, value, temporal):
    if temporal:
        ref[:, :, start : start + 2 * HS] = value.reshape(TIMES, 8, 2 * HS).astype(BF16)
    else:
        ref[:, start : start + 2 * HS] = value.astype(BF16)


def attend_kernel(qkv_ref, mix_ref, *, temporal):
    width = mix_ref.shape[-1]
    rows = TIMES * 8 if temporal else mix_ref.shape[0]
    allowed = same_sequence(rows, temporal)
    for pair in range(width // (2 * HS)):
        at = pair * 2 * HS
        q = rows_of(qkv_ref, at, temporal)
        k = rows_of(qkv_ref, width + at, temporal)
        v = rows_of(qkv_ref, 2 * width + at, temporal)
        mixed = None
        for second in (False, True):
            lanes = head_lanes(rows, second)
            probs = softmax_of(jnp.where(lanes, q, 0), k, allowed).astype(BF16)
            part = dot(probs, jnp.where(lanes, v, 0), NN)
            mixed = part if mixed is None else mixed + part
        put_rows(mix_ref, at, mixed, temporal)


def attend_back_kernel(qkv_ref, mix_g_ref, qkv_g_ref, *, temporal):
    width = mix_g_ref.shape[-1]
    rows = TIMES * 8 if temporal else mix_g_ref.shape[0]
    allowed = same_sequence(rows, temporal)
    scale = HS ** -0.5
    for pair in range(width // (2 * HS)):
        at = pair * 2 * HS
        q = rows_of(qkv_ref, at, temporal)
        k = rows_of(qkv_ref, width + at, temporal)
        v = rows_of(qkv_ref, 2 * width + at, temporal)
        g = rows_of(mix_g_ref, at, temporal)
        total = [None, None, None]
        for second in (False, True):
            lanes = head_lanes(rows, second)
            q_one, g_one = jnp.where(lanes, q, 0), jnp.where(lanes, g, 0)
            probs = softmax_of(q_one, k, allowed)
            prob_g = dot(g_one, v, NT)
            inner = jnp.sum(prob_g * probs, axis=-1, keepdims=True)
            score_g = (probs * (prob_g - inner)).astype(BF16)
            parts = (
                dot(score_g, jnp.where(lanes, k, 0), NN),
                dot(score_g, q_one, TN),
                dot(probs.astype(BF16), g_one, TN),
            )
            total = [p if t is None else t + p for t, p in zip(total, parts)]
        put_rows(qkv_g_ref, at, total[0] * scale, temporal)
        put_rows(qkv_g_ref, width + at, total[1] * scale, temporal)
        put_rows(qkv_g_ref, 2 * width + at, total[2], temporal)


def attention_call(kernel, operands, out_width, temporal):
    total = operands[0].shape[0]
    if temporal:
        seqs = total // TIMES
        grid = (seqs // 8,)

        def spec(cols):
            return pl.BlockSpec((TIMES, 8, cols), lambda i: (0, i, 0))

        operands = [x.reshape(TIMES, seqs, x.shape[-1]) for x in operands]
        out_shape = (TIMES, seqs, out_width)
    else:
        rows = 4 * SLOT
        grid = (total // rows,)

        def spec(cols):
            return pl.BlockSpec((rows, cols), lambda i: (i, 0))

        out_shape = (total, out_width)
    rows = 128 if temporal else 4 * SLOT
    dots = 2 if len(operands) == 1 else 5
    out = pl.pallas_call(
        functools.partial(kernel, temporal=temporal),
        grid=grid,
        in_specs=[spec(x.shape[-1]) for x in operands],
        out_specs=spec(out_width),
        out_shape=jax.ShapeDtypeStruct(out_shape, BF16),
        cost_estimate=pl.CostEstimate(
            flops=dots * grid[0] * 12 * rows * rows * 256,
            bytes_accessed=2 * total * (out_width + sum(x.shape[-1] for x in operands)),
            transcendentals=grid[0] * 12 * rows * rows,
        ),
    )(*operands)
    return out.reshape(total, out_width)


class Copies:
    def __init__(self, send_sems, recv_sems):
        self.send_sems, self.recv_sems, self.made = send_sems, recv_sems, []

    def start(self, source, target, device):
        at = len(self.made)
        copy = pltpu.make_async_remote_copy(
            src_ref=source, dst_ref=target, send_sem=self.send_sems.at[at],
            recv_sem=self.recv_sems.at[at], device_id=device,
            device_id_type=pl.DeviceIdType.MESH,
        )
        copy.start()
        self.made.append(copy)
        return copy


def here():
    a = lax.axis_index("a")
    z = 2 * lax.axis_index("b") + lax.axis_index("c")
    core, x, y = a % 2, (a // 2) % 2, a // 4
    flips = {1: 1 - 2 * core, 2: 2 - 4 * x, 4: 4 - 8 * y, 0: 0}

    def part(mask):
        return a + flips[mask & 1] + flips[mask & 2] + flips[mask & 4]

    return a, z, part


def plane(part, mask):
    return {"a": part(mask)}


def column(z):
    return {"b": z // 2, "c": z % 2}


def greet(part, z):
    barrier = pltpu.get_barrier_semaphore()
    for device in [plane(part, m) for m in (1, 2, 4)] + [column((z + j) % 4) for j in (1, 2, 3)]:
        pl.semaphore_signal(barrier, inc=1, device_id=device, device_id_type=pl.DeviceIdType.MESH)
    pl.semaphore_wait(barrier, 6)


def gather_kernel(*refs, count):
    shards, fulls = refs[:count], refs[count : 2 * count]
    staging = refs[2 * count : 3 * count]
    send_sems, recv_sems, local_sems = refs[3 * count :]
    me, z, part = here()
    loads = [
        pltpu.make_async_copy(shards[w], staging[w], local_sems.at[w]) for w in range(count)
    ]
    for load in loads:
        load.start()
    greet(part, z)
    copies = Copies(send_sems, recv_sems)
    items = []
    for w in range(count):
        for j in (1, 2, 3):
            sent = copies.start(
                shards[w].at[:, me], fulls[w].at[:, z, me], column((z + j) % 4)
            )
            items.append((w, (z + 4 - j) % 4, sent))
    stores = []
    for w in range(count):
        loads[w].wait()
        store = pltpu.make_async_copy(staging[w], fulls[w].at[:, z], local_sems.at[count + w])
        store.start()
        stores.append(store)
    total, lag = len(items), 3
    from_x, from_y, from_far, from_core = {}, {}, {}, []

    def push(w, zz, mask, to):
        at = part(mask)
        return copies.start(fulls[w].at[:, zz, at], fulls[w].at[:, zz, at], plane(part, to))

    for step in range(total + 2 * lag):
        if step < total:
            w, zz, sent = items[step]
            sent.wait_recv()
            from_x[step] = push(w, zz, 0, 2)
            from_y[step] = push(w, zz, 0, 4)
            from_core.append(push(w, zz, 0, 1))
        late = step - lag
        if 0 <= late < total:
            w, zz, _ = items[late]
            from_x[late].wait_recv()
            if late % 2 == 0:
                from_far[late] = push(w, zz, 2, 4)
            from_core.append(push(w, zz, 2, 1))
            from_y[late].wait_recv()
            if late % 2 == 1:
                from_far[late] = push(w, zz, 4, 2)
            from_core.append(push(w, zz, 4, 1))
        last = step - 2 * lag
        if 0 <= last < total:
            w, zz, _ = items[last]
            from_far[last].wait_recv()
            from_core.append(push(w, zz, 6, 1))
    for copy in from_core:
        copy.wait_recv()
    for copy in copies.made:
        copy.wait_send()
    for store in stores:
        store.wait()


def gather_weights(shards, dp, tp):
    count = len(shards)
    views = [x.reshape(x.shape[0], dp, x.shape[1] // dp, x.shape[2]) for x in shards]
    anywhere = pl.BlockSpec(memory_space=pl.ANY)
    sent = sum(x.size for x in shards) * 2
    fulls = pl.pallas_call(
        functools.partial(gather_kernel, count=count),
        out_shape=[
            jax.ShapeDtypeStruct((v.shape[0], tp) + v.shape[1:], v.dtype) for v in views
        ],
        in_specs=[anywhere] * count,
        out_specs=[anywhere] * count,
        scratch_shapes=[pltpu.VMEM(v.shape, v.dtype) for v in views]
        + [
            pltpu.SemaphoreType.DMA((count * 27,)),
            pltpu.SemaphoreType.DMA((count * 27,)),
            pltpu.SemaphoreType.DMA((2 * count,)),
        ],
        compiler_params=pltpu.CompilerParams(collective_id=0, has_side_effects=True),
        cost_estimate=pl.CostEstimate(flops=0, bytes_accessed=40 * sent, transcendentals=0),
        name="gather_weights",
    )(*views)
    return [f.reshape(f.shape[0], -1, f.shape[-1]) for f in fulls]


def build(mesh):
    dp, tp = mesh.shape["dp"], mesh.shape["tensor"]
    count = dp * tp
    groups = count // TIMES
    if groups <= tp:
        shape = (dp, tp // groups, groups)
        names = dict(time=("a", "b"), tensor=("b", "c"), dp=("a",))
    else:
        shape = (TIMES, groups // tp, tp)
        names = dict(time=("a",), tensor=("c",), dp=("a", "b"))
    inner = Mesh(mesh.devices.reshape(shape), ("a", "b", "c"))
    return inner, names, dp, tp


def make_device(names, dp, tp):
    every = ("a", "b", "c")

    def regroup(x):
        return lax.all_to_all(x, names["time"], split_axis=0, concat_axis=0, tiled=True)

    def gather_all(piece):
        full = lax.all_gather(piece, every, axis=0, tiled=False)
        return full.reshape((dp, tp) + piece.shape)

    def per_device(
        tokens, space_gain, space_shift, space_inproj, space_bias, space_outproj,
        space_outbias, time_gain, time_shift, time_inproj, time_bias, time_outproj,
        time_outbias, feed_gain, feed_shift, up_weight, up_bias, down_weight,
        down_bias, cotangent,
    ):
        width = tokens.shape[-1]
        own = tokens.shape[0] * tokens.shape[1]
        heads_width = space_inproj.shape[2]
        units = up_weight.shape[0]
        d_index = lax.axis_index(names["dp"])
        k_index = lax.axis_index(names["tensor"])
        hp, up = heads_width // dp, units // dp

        def piece_of(rows, per):
            return lax.dynamic_slice_in_dim(rows, d_index * per, per, rows.ndim - 2)

        def attn_piece(inproj, outproj):
            in_piece = piece_of(inproj.transpose(1, 2, 0), hp).reshape(3 * hp, width)
            return jnp.concatenate([in_piece, piece_of(outproj, hp)], axis=0)

        def attn_full(full):
            w_in = full[:, :, : 3 * hp].reshape(dp, tp, 3, hp, width)
            w_in = w_in.transpose(2, 1, 0, 3, 4).reshape(3 * width, width)
            w_out = full[:, :, 3 * hp : 4 * hp].transpose(1, 0, 2, 3).reshape(width, width)
            return w_in, w_out

        def in_rows(inproj):
            return inproj.transpose(1, 2, 0)

        if (dp, tp) == (8, 4):
            space_in_w, space_out_w, time_in_w, time_out_w = [
                w.reshape(-1, width)
                for w in gather_weights(
                    [in_rows(space_inproj), space_outproj[None], in_rows(time_inproj), time_outproj[None]],
                    dp, tp,
                )
            ]
        else:
            space_in_w, space_out_w = attn_full(gather_all(attn_piece(space_inproj, space_outproj)))
            time_in_w, time_out_w = attn_full(gather_all(attn_piece(time_inproj, time_outproj)))
        full_feed = gather_all(
            jnp.concatenate([piece_of(up_weight, up), piece_of(down_weight, up)], axis=0)
        )
        up_w = full_feed[:, :, :up].reshape(dp * tp * up, width)
        down_w = full_feed[:, :, up:].reshape(dp * tp * up, width)
        biases = lax.all_gather(
            jnp.concatenate([up_bias, space_bias.reshape(-1), time_bias.reshape(-1)]),
            names["tensor"], axis=0, tiled=False,
        ).astype(F32)
        up_b = biases[:, :units].reshape(tp, dp, up).transpose(1, 0, 2).reshape(-1)

        def in_bias(start):
            pair = biases[:, start : start + 2 * heads_width].reshape(tp, 2, heads_width)
            pair = pair.transpose(1, 0, 2).reshape(2, width)
            return jnp.concatenate([pair[0], jnp.zeros((width,), F32), pair[1]])

        space_b, time_b = in_bias(units), in_bias(units + 2 * heads_width)

        seqs = own // TIMES
        slots = TIMES * SLOT

        def pad_rows(x):
            x = x.reshape(TIMES, seqs, width)
            return jnp.pad(x, ((0, 0), (0, SLOT - seqs), (0, 0))).reshape(slots, width)

        def unpad(x):
            return x.reshape(TIMES, SLOT, width)[:, :seqs].reshape(tokens.shape)

        def exchange(x):
            return regroup(x.reshape(TIMES, SLOT, width)).reshape(slots, width)

        cot = exchange(pad_rows(cotangent))

        resid = pad_rows(tokens).astype(F32)
        space_n, space_r = norm_stats(resid)
        space_in = (space_n * space_gain + space_shift).astype(BF16)
        space_qkv = (dot(space_in, space_in_w, NT) + space_b).astype(BF16)
        space_mix = attention_call(attend_kernel, [space_qkv], width, False)
        after_space = resid + dot(space_mix, space_out_w, NN) + space_outbias.astype(F32)
        tn, _ = norm_stats(after_space)
        time_in_own = (tn * time_gain + time_shift).astype(BF16)

        time_in = exchange(time_in_own)
        after_space_p = exchange(after_space)
        time_qkv = (dot(time_in, time_in_w, NT) + time_b).astype(BF16)
        time_mix = attention_call(attend_kernel, [time_qkv], width, True)
        after_time = after_space_p + dot(time_mix, time_out_w, NN) + time_outbias.astype(F32)
        feed_n, feed_r = norm_stats(after_time)
        feed_in = (feed_n * feed_gain + feed_shift).astype(BF16)
        pre = dot(feed_in, up_w, NT) + up_b
        hidden = gelu_exact(pre).astype(BF16)
        layer_p = (after_time + dot(hidden, down_w, NN) + down_bias.astype(F32)).astype(BF16)
        layer_out = unpad(exchange(layer_p))

        upstream = cot.astype(F32)
        down_bias_g = jnp.sum(upstream, axis=0)
        down_g = dot(hidden, cot, TN).astype(BF16)
        pre_g = (dot(cot, down_w, NT) * gelu_slope(pre)).astype(BF16)
        up_g = dot(pre_g, feed_in, TN).astype(BF16)
        up_bias_g = jnp.sum(pre_g.astype(F32), axis=0)
        feed_g = dot(pre_g, up_w, NN)
        feed_gain_g = jnp.sum(feed_g * feed_n, axis=0)
        feed_shift_g = jnp.sum(feed_g, axis=0)
        after_time_g = upstream + norm_back(feed_g, feed_n, feed_r, feed_gain)

        def scatter(grad):
            return lax.psum_scatter(grad, every, scatter_dimension=0, tiled=False)

        feed_pack = jnp.concatenate(
            [up_g.reshape(dp * tp, up, width), down_g.reshape(dp * tp, up, width)], axis=1
        )
        feed_pack, after_time_g = lax.optimization_barrier((feed_pack, after_time_g))
        feed_part = scatter(feed_pack)

        def attention_back(branch, normed_in, qkv, mix, w_in, w_out, temporal):
            outbias_g = jnp.sum(branch.astype(F32), axis=0)
            mix_g = dot(branch, w_out, NT).astype(BF16)
            qkv_g = attention_call(attend_back_kernel, [qkv, mix_g], 3 * width, temporal)
            normed_g = dot(qkv_g, w_in, NN)
            return normed_g, qkv_g, outbias_g

        def attention_weights(branch, normed_in, mix, qkv_g):
            sums = jnp.sum(qkv_g.astype(F32), axis=0).reshape(3, width)
            out_g = dot(mix, branch, TN).astype(BF16)
            in_g = dot(qkv_g, normed_in, TN).astype(BF16)
            pack = jnp.concatenate(
                [
                    in_g.reshape(3, tp, dp, hp, width)
                    .transpose(2, 1, 0, 3, 4)
                    .reshape(dp * tp, 3 * hp, width),
                    out_g.reshape(tp, dp, hp, width)
                    .transpose(1, 0, 2, 3)
                    .reshape(dp * tp, hp, width),
                ],
                axis=1,
            )
            return pack, sums

        time_branch = after_time_g.astype(BF16)
        time_in_g, time_qkv_g, time_outbias_g = attention_back(
            time_branch, time_in, time_qkv, time_mix, time_in_w, time_out_w, True
        )
        tn_p, tr_p = norm_stats(after_space_p)
        time_gain_g = jnp.sum(time_in_g * tn_p, axis=0)
        time_shift_g = jnp.sum(time_in_g, axis=0)
        after_space_g_p = after_time_g + norm_back(time_in_g, tn_p, tr_p, time_gain)

        high_p = after_space_g_p.astype(BF16)
        low_p = (after_space_g_p - high_p.astype(F32)).astype(BF16)
        high = exchange(high_p)
        low = exchange(low_p)
        time_pack, time_sums = attention_weights(time_branch, time_in, time_mix, time_qkv_g)
        after_space_g = high.astype(F32) + low.astype(F32)

        space_in_g, space_qkv_g, space_outbias_g = attention_back(
            high, space_in, space_qkv, space_mix, space_in_w, space_out_w, False
        )
        space_pack, space_sums = attention_weights(high, space_in, space_mix, space_qkv_g)
        attn_part = scatter(jnp.concatenate([time_pack, space_pack], axis=1))
        space_gain_g = jnp.sum(space_in_g * space_n, axis=0)
        space_shift_g = jnp.sum(space_in_g, axis=0)
        input_g = unpad(after_space_g + norm_back(space_in_g, space_n, space_r, space_gain))

        small = jnp.concatenate(
            [
                space_gain_g, space_shift_g, space_outbias_g, time_gain_g, time_shift_g,
                time_outbias_g, feed_gain_g, feed_shift_g, down_bias_g,
                space_sums[0], space_sums[2], time_sums[0], time_sums[2],
                up_bias_g.reshape(dp, tp, up).transpose(1, 0, 2).reshape(-1),
            ]
        )
        small = lax.psum(small, every)
        rows = small[: 13 * width].reshape(13, width)
        head_rows = lax.dynamic_slice_in_dim(rows[9:], k_index * heads_width, heads_width, 1)
        up_bias_out = lax.dynamic_slice_in_dim(small[13 * width :], k_index * units, units, 0)

        def spread(part):
            return lax.all_gather(part, names["dp"], axis=0, tiled=False)

        def attn_out(full):
            in_out = full[:, : 3 * hp].reshape(dp, 3, hp, width).transpose(1, 0, 2, 3)
            in_out = in_out.reshape(3, heads_width, width).transpose(2, 0, 1).astype(F32)
            return in_out, full[:, 3 * hp :].reshape(heads_width, width).astype(F32)

        feed_all = spread(feed_part)
        attn_all = spread(attn_part)
        time_in_out, time_out_out = attn_out(attn_all[:, : 4 * hp])
        space_in_out, space_out_out = attn_out(attn_all[:, 4 * hp :])
        return (
            layer_out,
            input_g,
            rows[0], rows[1], space_in_out, head_rows[0:2], space_out_out, rows[2],
            rows[3], rows[4], time_in_out, head_rows[2:4], time_out_out, rows[5],
            rows[6], rows[7],
            feed_all[:, :up].reshape(units, width).astype(F32),
            up_bias_out,
            feed_all[:, up:].reshape(units, width).astype(F32),
            rows[8],
        )

    return per_device


def solution(mesh):
    inner, names, dp, tp = build(mesh)
    every, tensor = ("a", "b", "c"), names["tensor"]
    frames = P(every, None, None)
    head_in = P(None, None, tensor)
    head_bias = P(None, tensor)
    row = P(tensor, None)
    return jax.shard_map(
        make_device(names, dp, tp),
        mesh=inner,
        in_specs=(
            frames, P(), P(), head_in, head_bias, row, P(),
            P(), P(), head_in, head_bias, row, P(),
            P(), P(), row, P(tensor), row, P(), frames,
        ),
        out_specs=(
            frames, frames, P(), P(), head_in, head_bias, row, P(),
            P(), P(), head_in, head_bias, row, P(),
            P(), P(), row, P(tensor), row, P(),
        ),
        check_vma=False,
    )
```

```python
import functools

import jax
import jax.numpy as jnp
from jax import lax
from jax.experimental import pallas as pl
from jax.experimental.pallas import tpu as pltpu
from jax.sharding import Mesh, PartitionSpec as P

HS = 64
PATCH = 196
TIMES = 16
SLOT = 56
EPSILON = 1e-06
ROOT_HALF = 0.7071067811865476
INV_ROOT_TAU = 0.3989422804014327
F32 = jnp.float32
BF16 = jnp.bfloat16
NT = (((1,), (1,)), ((), ()))
NN = (((1,), (0,)), ((), ()))
TN = (((0,), (0,)), ((), ()))


def dot(a, b, dims):
    return lax.dot_general(a, b, dims, preferred_element_type=F32)


def norm_stats(values):
    center = values - jnp.mean(values, axis=-1, keepdims=True)
    second = jnp.mean(center * center, axis=-1, keepdims=True)
    rate = lax.rsqrt(second + EPSILON)
    return center * rate, rate


def norm_back(grad, normed, rate, gain):
    e = grad * gain
    inner = jnp.mean(e * normed, axis=-1, keepdims=True)
    return rate * (e - jnp.mean(e, axis=-1, keepdims=True) - normed * inner)


def gelu_exact(values):
    return 0.5 * values * (1.0 + lax.erf(values * ROOT_HALF))


def gelu_slope(values):
    return (
        0.5 * (1.0 + lax.erf(values * ROOT_HALF))
        + values * jnp.exp(-0.5 * values * values) * INV_ROOT_TAU
    )


def same_sequence(rows, temporal):
    r = lax.broadcasted_iota(jnp.int32, (rows, rows), 0)
    c = lax.broadcasted_iota(jnp.int32, (rows, rows), 1)
    if temporal:
        return (r % 8) == (c % 8)
    return (c % SLOT) < (PATCH // 4)


def head_lanes(rows, second):
    lane = lax.broadcasted_iota(jnp.int32, (rows, 2 * HS), 1)
    return (lane >= HS) if second else (lane < HS)


def softmax_of(q_one, k_pair, allowed):
    scores = dot(q_one, k_pair, NT) * (HS ** -0.5)
    scores = jnp.where(allowed, scores, -1e30)
    top = jnp.max(scores, axis=-1, keepdims=True)
    weights = jnp.exp(scores - top)
    return weights / jnp.sum(weights, axis=-1, keepdims=True)


def rows_of(ref, start, temporal):
    if temporal:
        block = ref[:, :, start : start + 2 * HS].astype(F32)
        return block.reshape(-1, 2 * HS).astype(BF16)
    return ref[:, start : start + 2 * HS]


def put_rows(ref, start, value, temporal):
    if temporal:
        ref[:, :, start : start + 2 * HS] = value.reshape(TIMES, 8, 2 * HS).astype(BF16)
    else:
        ref[:, start : start + 2 * HS] = value.astype(BF16)


def attend_kernel(qkv_ref, mix_ref, *, temporal):
    width = mix_ref.shape[-1]
    rows = TIMES * 8 if temporal else mix_ref.shape[0]
    allowed = same_sequence(rows, temporal)
    for pair in range(width // (2 * HS)):
        at = pair * 2 * HS
        q = rows_of(qkv_ref, at, temporal)
        k = rows_of(qkv_ref, width + at, temporal)
        v = rows_of(qkv_ref, 2 * width + at, temporal)
        mixed = None
        for second in (False, True):
            lanes = head_lanes(rows, second)
            probs = softmax_of(jnp.where(lanes, q, 0), k, allowed).astype(BF16)
            part = dot(probs, jnp.where(lanes, v, 0), NN)
            mixed = part if mixed is None else mixed + part
        put_rows(mix_ref, at, mixed, temporal)


def attend_back_kernel(qkv_ref, mix_g_ref, qkv_g_ref, *, temporal):
    width = mix_g_ref.shape[-1]
    rows = TIMES * 8 if temporal else mix_g_ref.shape[0]
    allowed = same_sequence(rows, temporal)
    scale = HS ** -0.5
    for pair in range(width // (2 * HS)):
        at = pair * 2 * HS
        q = rows_of(qkv_ref, at, temporal)
        k = rows_of(qkv_ref, width + at, temporal)
        v = rows_of(qkv_ref, 2 * width + at, temporal)
        g = rows_of(mix_g_ref, at, temporal)
        total = [None, None, None]
        for second in (False, True):
            lanes = head_lanes(rows, second)
            q_one, g_one = jnp.where(lanes, q, 0), jnp.where(lanes, g, 0)
            probs = softmax_of(q_one, k, allowed)
            prob_g = dot(g_one, v, NT)
            inner = jnp.sum(prob_g * probs, axis=-1, keepdims=True)
            score_g = (probs * (prob_g - inner)).astype(BF16)
            parts = (
                dot(score_g, jnp.where(lanes, k, 0), NN),
                dot(score_g, q_one, TN),
                dot(probs.astype(BF16), g_one, TN),
            )
            total = [p if t is None else t + p for t, p in zip(total, parts)]
        put_rows(qkv_g_ref, at, total[0] * scale, temporal)
        put_rows(qkv_g_ref, width + at, total[1] * scale, temporal)
        put_rows(qkv_g_ref, 2 * width + at, total[2], temporal)


def attention_call(kernel, operands, out_width, temporal):
    total = operands[0].shape[0]
    if temporal:
        seqs = total // TIMES
        grid = (seqs // 8,)

        def spec(cols):
            return pl.BlockSpec((TIMES, 8, cols), lambda i: (0, i, 0))

        operands = [x.reshape(TIMES, seqs, x.shape[-1]) for x in operands]
        out_shape = (TIMES, seqs, out_width)
    else:
        rows = 4 * SLOT
        grid = (total // rows,)

        def spec(cols):
            return pl.BlockSpec((rows, cols), lambda i: (i, 0))

        out_shape = (total, out_width)
    rows = 128 if temporal else 4 * SLOT
    dots = 2 if len(operands) == 1 else 5
    out = pl.pallas_call(
        functools.partial(kernel, temporal=temporal),
        grid=grid,
        in_specs=[spec(x.shape[-1]) for x in operands],
        out_specs=spec(out_width),
        out_shape=jax.ShapeDtypeStruct(out_shape, BF16),
        cost_estimate=pl.CostEstimate(
            flops=dots * grid[0] * 12 * rows * rows * 256,
            bytes_accessed=2 * total * (out_width + sum(x.shape[-1] for x in operands)),
            transcendentals=grid[0] * 12 * rows * rows,
        ),
    )(*operands)
    return out.reshape(total, out_width)


class Copies:
    def __init__(self, send_sems, recv_sems):
        self.send_sems, self.recv_sems, self.made = send_sems, recv_sems, []

    def start(self, source, target, device):
        at = len(self.made)
        copy = pltpu.make_async_remote_copy(
            src_ref=source, dst_ref=target, send_sem=self.send_sems.at[at],
            recv_sem=self.recv_sems.at[at], device_id=device,
            device_id_type=pl.DeviceIdType.MESH,
        )
        copy.start()
        self.made.append(copy)
        return copy


def here():
    a = lax.axis_index("a")
    z = 2 * lax.axis_index("b") + lax.axis_index("c")
    core, x, y = a % 2, (a // 2) % 2, a // 4
    flips = {1: 1 - 2 * core, 2: 2 - 4 * x, 4: 4 - 8 * y, 0: 0}

    def part(mask):
        return a + flips[mask & 1] + flips[mask & 2] + flips[mask & 4]

    return a, z, part


def plane(part, mask):
    return {"a": part(mask)}


def column(z):
    return {"b": z // 2, "c": z % 2}


def greet(part, z):
    barrier = pltpu.get_barrier_semaphore()
    for device in [plane(part, m) for m in (1, 2, 4)] + [column((z + j) % 4) for j in (1, 2, 3)]:
        pl.semaphore_signal(barrier, inc=1, device_id=device, device_id_type=pl.DeviceIdType.MESH)
    pl.semaphore_wait(barrier, 6)


def gather_kernel(*refs, count):
    shards, fulls = refs[:count], refs[count : 2 * count]
    staging = refs[2 * count : 3 * count]
    send_sems, recv_sems, local_sems = refs[3 * count :]
    me, z, part = here()
    loads = [
        pltpu.make_async_copy(shards[w], staging[w], local_sems.at[w]) for w in range(count)
    ]
    for load in loads:
        load.start()
    greet(part, z)
    copies = Copies(send_sems, recv_sems)
    items = []
    for w in range(count):
        for j in (1, 2, 3):
            sent = copies.start(
                shards[w].at[:, me], fulls[w].at[:, z, me], column((z + j) % 4)
            )
            items.append((w, (z + 4 - j) % 4, sent))
    stores = []
    for w in range(count):
        loads[w].wait()
        store = pltpu.make_async_copy(staging[w], fulls[w].at[:, z], local_sems.at[count + w])
        store.start()
        stores.append(store)
    total, lag = len(items), 3
    from_x, from_y, from_far, from_core = {}, {}, {}, []

    def push(w, zz, mask, to):
        at = part(mask)
        return copies.start(fulls[w].at[:, zz, at], fulls[w].at[:, zz, at], plane(part, to))

    for step in range(total + 2 * lag):
        if step < total:
            w, zz, sent = items[step]
            sent.wait_recv()
            from_x[step] = push(w, zz, 0, 2)
            from_y[step] = push(w, zz, 0, 4)
            from_core.append(push(w, zz, 0, 1))
        late = step - lag
        if 0 <= late < total:
            w, zz, _ = items[late]
            from_x[late].wait_recv()
            if late % 2 == 0:
                from_far[late] = push(w, zz, 2, 4)
            from_core.append(push(w, zz, 2, 1))
            from_y[late].wait_recv()
            if late % 2 == 1:
                from_far[late] = push(w, zz, 4, 2)
            from_core.append(push(w, zz, 4, 1))
        last = step - 2 * lag
        if 0 <= last < total:
            w, zz, _ = items[last]
            from_far[last].wait_recv()
            from_core.append(push(w, zz, 6, 1))
    for copy in from_core:
        copy.wait_recv()
    for copy in copies.made:
        copy.wait_send()
    for store in stores:
        store.wait()


def gather_weights(shards, dp, tp):
    count = len(shards)
    views = [x.reshape(x.shape[0], dp, x.shape[1] // dp, x.shape[2]) for x in shards]
    anywhere = pl.BlockSpec(memory_space=pl.ANY)
    sent = sum(x.size for x in shards) * 2
    fulls = pl.pallas_call(
        functools.partial(gather_kernel, count=count),
        out_shape=[
            jax.ShapeDtypeStruct((v.shape[0], tp) + v.shape[1:], v.dtype) for v in views
        ],
        in_specs=[anywhere] * count,
        out_specs=[anywhere] * count,
        scratch_shapes=[pltpu.VMEM(v.shape, v.dtype) for v in views]
        + [
            pltpu.SemaphoreType.DMA((count * 27,)),
            pltpu.SemaphoreType.DMA((count * 27,)),
            pltpu.SemaphoreType.DMA((2 * count,)),
        ],
        compiler_params=pltpu.CompilerParams(collective_id=0, has_side_effects=True),
        cost_estimate=pl.CostEstimate(flops=0, bytes_accessed=40 * sent, transcendentals=0),
        name="gather_weights",
    )(*views)
    return [f.reshape(f.shape[0], -1, f.shape[-1]) for f in fulls]


BLOCKS = (6, 2, 4, 0)


def add_into(target, source):
    def step(i, carry):
        target[i] = (target[i].astype(F32) + source[i].astype(F32)).astype(BF16)
        return carry

    lax.fori_loop(0, target.shape[0], step, 0)


def scatter_kernel(*refs):
    packs, outs = refs[0:2], refs[2:4]
    accs, cores, firsts, seconds, columns = (refs[4 + 2 * i : 6 + 2 * i] for i in range(5))
    send_sems, recv_sems, local_sems = refs[14:]
    me, z, part = here()
    loads = {}
    for b, mask in enumerate(BLOCKS):
        for s in (0, 1):
            loads[s, mask] = pltpu.make_async_copy(
                packs[s].at[part(mask)], accs[s].at[b], local_sems.at[2 * b + s]
            )
            loads[s, mask].start()
    greet(part, z)
    copies = Copies(send_sems, recv_sems)
    first_core = {}
    for b, mask in enumerate(BLOCKS):
        for s in (0, 1):
            first_core[s, mask] = copies.start(
                packs[s].at[part(mask ^ 1)], cores[s].at[b], plane(part, 1)
            )
    near, far = (2, 4), (4, 2)
    hop = {}
    for b, mask in enumerate(BLOCKS):
        for s in (0, 1):
            loads[s, mask].wait()
            first_core[s, mask].wait_recv()
            add_into(accs[s].at[b], cores[s].at[b])
        for s in (0, 1):
            if mask & near[s]:
                slot = 0 if mask == 6 else 1
                hop[s, slot] = copies.start(
                    accs[s].at[b], firsts[s].at[slot], plane(part, near[s])
                )
    for s in (0, 1):
        b = BLOCKS.index(far[s])
        hop[s, 0].wait_recv()
        add_into(accs[s].at[b], firsts[s].at[0])
    for s in (0, 1):
        b = BLOCKS.index(far[s])
        hop[s, 2] = copies.start(accs[s].at[b], seconds[s], plane(part, far[s]))
    for s in (0, 1):
        hop[s, 1].wait_recv()
        add_into(accs[s].at[3], firsts[s].at[1])
    lines = {}
    for s in (0, 1):
        hop[s, 2].wait_recv()
        add_into(accs[s].at[3], seconds[s])
    for s in (0, 1):
        for j in (1, 2, 3):
            to = (z + j) % 4
            lines[s, j] = copies.start(accs[s].at[3, to], columns[s].at[j - 1], column(to))
    for s in (0, 1):
        total = accs[s][3, z].astype(F32)
        for j in (1, 2, 3):
            lines[s, j].wait_recv()
            total = total + columns[s][j - 1].astype(F32)
        outs[s][me] = total.astype(BF16)

    def push(s, mask, to):
        at = part(mask)
        return copies.start(outs[s].at[at], outs[s].at[at], plane(part, to))

    ends = []
    along = {}
    for s in (0, 1):
        along[s, 2] = push(s, 0, 2)
        along[s, 4] = push(s, 0, 4)
        ends.append(push(s, 0, 1))
    relays = []
    for s in (0, 1):
        for mask in (2, 4):
            along[s, mask].wait_recv()
            if mask == near[s]:
                relays.append((s, push(s, mask, far[s])))
            ends.append(push(s, mask, 1))
    for s, copy in relays:
        copy.wait_recv()
        ends.append(push(s, 6, 1))
    for copy in ends:
        copy.wait_recv()
    for copy in copies.made:
        copy.wait_send()


def scatter_sum(packs):
    count = 2 * (4 + 3 + 3 + 3 + 4)
    anywhere = pl.BlockSpec(memory_space=pl.ANY)
    rows = [p.shape[2:] for p in packs]

    def scratch(*lead):
        return [pltpu.VMEM(lead + r, BF16) for r in rows]

    return pl.pallas_call(
        scatter_kernel,
        out_shape=[jax.ShapeDtypeStruct((8,) + r, BF16) for r in rows],
        in_specs=[anywhere] * 2,
        out_specs=[pl.BlockSpec(memory_space=pltpu.VMEM)] * 2,
        scratch_shapes=scratch(4, 4) + scratch(4, 4) + scratch(2, 4) + scratch(4) + scratch(3)
        + [
            pltpu.SemaphoreType.DMA((count,)),
            pltpu.SemaphoreType.DMA((count,)),
            pltpu.SemaphoreType.DMA((8,)),
        ],
        compiler_params=pltpu.CompilerParams(collective_id=1, has_side_effects=True),
        cost_estimate=pl.CostEstimate(flops=0, bytes_accessed=300000000, transcendentals=0),
        name="scatter_sum",
    )(*packs)


def build(mesh):
    dp, tp = mesh.shape["dp"], mesh.shape["tensor"]
    count = dp * tp
    groups = count // TIMES
    if groups <= tp:
        shape = (dp, tp // groups, groups)
        names = dict(time=("a", "b"), tensor=("b", "c"), dp=("a",))
    else:
        shape = (TIMES, groups // tp, tp)
        names = dict(time=("a",), tensor=("c",), dp=("a", "b"))
    inner = Mesh(mesh.devices.reshape(shape), ("a", "b", "c"))
    return inner, names, dp, tp


def make_device(names, dp, tp):
    every = ("a", "b", "c")

    def regroup(x):
        return lax.all_to_all(x, names["time"], split_axis=0, concat_axis=0, tiled=True)

    def gather_all(piece):
        full = lax.all_gather(piece, every, axis=0, tiled=False)
        return full.reshape((dp, tp) + piece.shape)

    def per_device(
        tokens, space_gain, space_shift, space_inproj, space_bias, space_outproj,
        space_outbias, time_gain, time_shift, time_inproj, time_bias, time_outproj,
        time_outbias, feed_gain, feed_shift, up_weight, up_bias, down_weight,
        down_bias, cotangent,
    ):
        width = tokens.shape[-1]
        own = tokens.shape[0] * tokens.shape[1]
        heads_width = space_inproj.shape[2]
        units = up_weight.shape[0]
        d_index = lax.axis_index(names["dp"])
        k_index = lax.axis_index(names["tensor"])
        hp, up = heads_width // dp, units // dp

        def piece_of(rows, per):
            return lax.dynamic_slice_in_dim(rows, d_index * per, per, rows.ndim - 2)

        def attn_piece(inproj, outproj):
            in_piece = piece_of(inproj.transpose(1, 2, 0), hp).reshape(3 * hp, width)
            return jnp.concatenate([in_piece, piece_of(outproj, hp)], axis=0)

        def attn_full(full):
            w_in = full[:, :, : 3 * hp].reshape(dp, tp, 3, hp, width)
            w_in = w_in.transpose(2, 1, 0, 3, 4).reshape(3 * width, width)
            w_out = full[:, :, 3 * hp : 4 * hp].transpose(1, 0, 2, 3).reshape(width, width)
            return w_in, w_out

        def in_rows(inproj):
            return inproj.transpose(1, 2, 0)

        direct = (dp, tp) == (8, 4)
        bias_shard = jnp.concatenate([up_bias, space_bias.reshape(-1), time_bias.reshape(-1)])
        per_row = bias_shard.shape[0] // dp
        if direct:
            bias_rows = jnp.pad(
                bias_shard.reshape(dp, 1, per_row), ((0, 0), (0, 7), (0, width - per_row))
            )
            space_in_w, space_out_w, time_in_w, time_out_w, bias_full = [
                w.reshape(-1, width)
                for w in gather_weights(
                    [
                        in_rows(space_inproj), space_outproj[None], in_rows(time_inproj),
                        time_outproj[None], bias_rows.reshape(1, -1, width),
                    ],
                    dp, tp,
                )
            ]
            biases = bias_full.reshape(tp, dp, 8, width)[:, :, 0, :per_row].reshape(tp, -1)
        else:
            space_in_w, space_out_w = attn_full(gather_all(attn_piece(space_inproj, space_outproj)))
            time_in_w, time_out_w = attn_full(gather_all(attn_piece(time_inproj, time_outproj)))
            biases = lax.all_gather(bias_shard, names["tensor"], axis=0, tiled=False)
        biases = biases.astype(F32)
        full_feed = gather_all(
            jnp.concatenate([piece_of(up_weight, up), piece_of(down_weight, up)], axis=0)
        )
        up_w = full_feed[:, :, :up].reshape(dp * tp * up, width)
        down_w = full_feed[:, :, up:].reshape(dp * tp * up, width)
        up_b = biases[:, :units].reshape(tp, dp, up).transpose(1, 0, 2).reshape(-1)

        def in_bias(start):
            pair = biases[:, start : start + 2 * heads_width].reshape(tp, 2, heads_width)
            pair = pair.transpose(1, 0, 2).reshape(2, width)
            return jnp.concatenate([pair[0], jnp.zeros((width,), F32), pair[1]])

        space_b, time_b = in_bias(units), in_bias(units + 2 * heads_width)

        seqs = own // TIMES
        slots = TIMES * SLOT

        def pad_rows(x):
            x = x.reshape(TIMES, seqs, width)
            return jnp.pad(x, ((0, 0), (0, SLOT - seqs), (0, 0))).reshape(slots, width)

        def unpad(x):
            return x.reshape(TIMES, SLOT, width)[:, :seqs].reshape(tokens.shape)

        def exchange(x):
            return regroup(x.reshape(TIMES, SLOT, width)).reshape(slots, width)

        cot = exchange(pad_rows(cotangent))

        resid = pad_rows(tokens).astype(F32)
        space_n, space_r = norm_stats(resid)
        space_in = (space_n * space_gain + space_shift).astype(BF16)
        space_qkv = (dot(space_in, space_in_w, NT) + space_b).astype(BF16)
        space_mix = attention_call(attend_kernel, [space_qkv], width, False)
        after_space = resid + dot(space_mix, space_out_w, NN) + space_outbias.astype(F32)

        after_space_p = exchange(after_space.astype(BF16)).astype(F32)
        tn_p, tr_p = norm_stats(after_space_p)
        time_in = (tn_p * time_gain + time_shift).astype(BF16)
        time_qkv = (dot(time_in, time_in_w, NT) + time_b).astype(BF16)
        time_mix = attention_call(attend_kernel, [time_qkv], width, True)
        after_time = after_space_p + dot(time_mix, time_out_w, NN) + time_outbias.astype(F32)
        feed_n, feed_r = norm_stats(after_time)
        feed_in = (feed_n * feed_gain + feed_shift).astype(BF16)
        pre = dot(feed_in, up_w, NT) + up_b
        hidden = gelu_exact(pre).astype(BF16)
        layer_p = (after_time + dot(hidden, down_w, NN) + down_bias.astype(F32)).astype(BF16)
        layer_out = unpad(exchange(layer_p))

        upstream = cot.astype(F32)
        down_bias_g = jnp.sum(upstream, axis=0)
        down_g = dot(hidden, cot, TN).astype(BF16)
        pre_g = (dot(cot, down_w, NT) * gelu_slope(pre)).astype(BF16)
        up_g = dot(pre_g, feed_in, TN).astype(BF16)
        up_bias_g = jnp.sum(pre_g.astype(F32), axis=0)
        feed_g = dot(pre_g, up_w, NN)
        feed_gain_g = jnp.sum(feed_g * feed_n, axis=0)
        feed_shift_g = jnp.sum(feed_g, axis=0)
        after_time_g = upstream + norm_back(feed_g, feed_n, feed_r, feed_gain)

        def scatter(grad):
            return lax.psum_scatter(grad, every, scatter_dimension=0, tiled=False)

        feed_pack = jnp.concatenate(
            [up_g.reshape(dp * tp, up, width), down_g.reshape(dp * tp, up, width)], axis=1
        )
        feed_pack, after_time_g = lax.optimization_barrier((feed_pack, after_time_g))
        feed_part = scatter(feed_pack)

        def attention_back(branch, normed_in, qkv, mix, w_in, w_out, temporal):
            outbias_g = jnp.sum(branch.astype(F32), axis=0)
            mix_g = dot(branch, w_out, NT).astype(BF16)
            qkv_g = attention_call(attend_back_kernel, [qkv, mix_g], 3 * width, temporal)
            normed_g = dot(qkv_g, w_in, NN)
            return normed_g, qkv_g, outbias_g

        def attention_weights(branch, normed_in, mix, qkv_g):
            sums = jnp.sum(qkv_g.astype(F32), axis=0).reshape(3, width)
            out_g = dot(mix, branch, TN).astype(BF16)
            in_g = dot(qkv_g, normed_in, TN).astype(BF16)
            pack = jnp.concatenate(
                [
                    in_g.reshape(3, tp, dp, hp, width)
                    .transpose(2, 1, 0, 3, 4)
                    .reshape(dp * tp, 3 * hp, width),
                    out_g.reshape(tp, dp, hp, width)
                    .transpose(1, 0, 2, 3)
                    .reshape(dp * tp, hp, width),
                ],
                axis=1,
            )
            return pack, sums

        time_branch = after_time_g.astype(BF16)
        time_in_g, time_qkv_g, time_outbias_g = attention_back(
            time_branch, time_in, time_qkv, time_mix, time_in_w, time_out_w, True
        )
        time_gain_g = jnp.sum(time_in_g * tn_p, axis=0)
        time_shift_g = jnp.sum(time_in_g, axis=0)
        after_space_g_p = after_time_g + norm_back(time_in_g, tn_p, tr_p, time_gain)

        high = exchange(after_space_g_p.astype(BF16))
        time_pack, time_sums = attention_weights(time_branch, time_in, time_mix, time_qkv_g)
        after_space_g = high.astype(F32)

        space_in_g, space_qkv_g, space_outbias_g = attention_back(
            high, space_in, space_qkv, space_mix, space_in_w, space_out_w, False
        )
        space_pack, space_sums = attention_weights(high, space_in, space_mix, space_qkv_g)
        space_gain_g = jnp.sum(space_in_g * space_n, axis=0)
        space_shift_g = jnp.sum(space_in_g, axis=0)
        input_g = unpad(after_space_g + norm_back(space_in_g, space_n, space_r, space_gain))

        shared = jnp.concatenate(
            [
                space_gain_g, space_shift_g, space_outbias_g, time_gain_g, time_shift_g,
                time_outbias_g, feed_gain_g, feed_shift_g, down_bias_g,
            ]
        )
        headed = jnp.stack([space_sums[0], space_sums[2], time_sums[0], time_sums[2]])
        headed = headed.reshape(4, tp, heads_width).transpose(1, 0, 2).reshape(tp, -1)
        upped = up_bias_g.reshape(dp, tp, up).transpose(1, 0, 2).reshape(tp, -1)
        sharded = jnp.concatenate([headed, upped], axis=1)
        many, few = 9 * width // dp, sharded.shape[1] // dp
        small = jnp.concatenate(
            [
                jnp.broadcast_to(shared.reshape(dp, 1, many), (dp, tp, many)),
                sharded.reshape(tp, dp, few).transpose(1, 0, 2),
                jnp.zeros((dp, tp, 2 * width - many - few), F32),
            ],
            axis=2,
        ).astype(BF16)
        small = jnp.pad(small.reshape(dp * tp, 2, width), ((0, 0), (0, 14), (0, 0)))
        space_pack = jnp.concatenate([space_pack, small], axis=1)

        def spread(part):
            return lax.all_gather(part, names["dp"], axis=0, tiled=False)

        if direct:
            time_all, space_all = scatter_sum(
                [x.reshape((dp, tp) + x.shape[1:]) for x in (time_pack, space_pack)]
            )
        else:
            both = spread(scatter(jnp.concatenate([time_pack, space_pack], axis=1)))
            time_all, space_all = both[:, : 4 * hp], both[:, 4 * hp :]

        def attn_out(full):
            in_out = full[:, : 3 * hp].reshape(dp, 3, hp, width).transpose(1, 0, 2, 3)
            in_out = in_out.reshape(3, heads_width, width).transpose(2, 0, 1).astype(F32)
            return in_out, full[:, 3 * hp : 4 * hp].reshape(heads_width, width).astype(F32)

        feed_all = spread(feed_part)
        time_in_out, time_out_out = attn_out(time_all)
        space_in_out, space_out_out = attn_out(space_all)
        sums = space_all[:, 4 * hp : 4 * hp + 2].reshape(dp, 2 * width).astype(F32)
        rows = sums[:, :many].reshape(9, width)
        own_sums = sums[:, many : many + few].reshape(-1)
        head_rows = own_sums[: 4 * heads_width].reshape(4, heads_width)
        up_bias_out = own_sums[4 * heads_width :]
        return (
            layer_out,
            input_g,
            rows[0], rows[1], space_in_out, head_rows[0:2], space_out_out, rows[2],
            rows[3], rows[4], time_in_out, head_rows[2:4], time_out_out, rows[5],
            rows[6], rows[7],
            feed_all[:, :up].reshape(units, width).astype(F32),
            up_bias_out,
            feed_all[:, up:].reshape(units, width).astype(F32),
            rows[8],
        )

    return per_device


def solution(mesh):
    inner, names, dp, tp = build(mesh)
    every, tensor = ("a", "b", "c"), names["tensor"]
    frames = P(every, None, None)
    head_in = P(None, None, tensor)
    head_bias = P(None, tensor)
    row = P(tensor, None)
    return jax.shard_map(
        make_device(names, dp, tp),
        mesh=inner,
        in_specs=(
            frames, P(), P(), head_in, head_bias, row, P(),
            P(), P(), head_in, head_bias, row, P(),
            P(), P(), row, P(tensor), row, P(), frames,
        ),
        out_specs=(
            frames, frames, P(), P(), head_in, head_bias, row, P(),
            P(), P(), head_in, head_bias, row, P(),
            P(), P(), row, P(tensor), row, P(),
        ),
        check_vma=False,
    )
```

```python
import functools

import jax
import jax.numpy as jnp
from jax import lax
from jax.experimental import pallas as pl
from jax.experimental.pallas import tpu as pltpu
from jax.sharding import Mesh, PartitionSpec as P

HS = 64
PATCH = 196
TIMES = 16
SLOT = 56
EPSILON = 1e-06
ROOT_HALF = 0.7071067811865476
INV_ROOT_TAU = 0.3989422804014327
F32 = jnp.float32
BF16 = jnp.bfloat16
NT = (((1,), (1,)), ((), ()))
NN = (((1,), (0,)), ((), ()))
TN = (((0,), (0,)), ((), ()))


def dot(a, b, dims):
    return lax.dot_general(a, b, dims, preferred_element_type=F32)


def norm_stats(values):
    center = values - jnp.mean(values, axis=-1, keepdims=True)
    second = jnp.mean(center * center, axis=-1, keepdims=True)
    rate = lax.rsqrt(second + EPSILON)
    return center * rate, rate


def norm_back(grad, normed, rate, gain):
    e = grad * gain
    inner = jnp.mean(e * normed, axis=-1, keepdims=True)
    return rate * (e - jnp.mean(e, axis=-1, keepdims=True) - normed * inner)


def gelu_exact(values):
    return 0.5 * values * (1.0 + lax.erf(values * ROOT_HALF))


def gelu_slope(values):
    return (
        0.5 * (1.0 + lax.erf(values * ROOT_HALF))
        + values * jnp.exp(-0.5 * values * values) * INV_ROOT_TAU
    )


def same_sequence(rows, temporal):
    r = lax.broadcasted_iota(jnp.int32, (rows, rows), 0)
    c = lax.broadcasted_iota(jnp.int32, (rows, rows), 1)
    if temporal:
        return (r % 8) == (c % 8)
    return (c % SLOT) < (PATCH // 4)


def head_lanes(rows, second):
    lane = lax.broadcasted_iota(jnp.int32, (rows, 2 * HS), 1)
    return (lane >= HS) if second else (lane < HS)


def softmax_of(q_one, k_pair, allowed):
    scores = dot(q_one, k_pair, NT) * (HS ** -0.5)
    scores = jnp.where(allowed, scores, -1e30)
    top = jnp.max(scores, axis=-1, keepdims=True)
    weights = jnp.exp(scores - top)
    return weights / jnp.sum(weights, axis=-1, keepdims=True)


def rows_of(ref, start, temporal):
    if temporal:
        block = ref[:, :, start : start + 2 * HS].astype(F32)
        return block.reshape(-1, 2 * HS).astype(BF16)
    return ref[:, start : start + 2 * HS]


def put_rows(ref, start, value, temporal):
    if temporal:
        ref[:, :, start : start + 2 * HS] = value.reshape(TIMES, 8, 2 * HS).astype(BF16)
    else:
        ref[:, start : start + 2 * HS] = value.astype(BF16)


def attend_kernel(qkv_ref, mix_ref, *, temporal):
    width = mix_ref.shape[-1]
    rows = TIMES * 8 if temporal else mix_ref.shape[0]
    allowed = same_sequence(rows, temporal)
    for pair in range(width // (2 * HS)):
        at = pair * 2 * HS
        q = rows_of(qkv_ref, at, temporal)
        k = rows_of(qkv_ref, width + at, temporal)
        v = rows_of(qkv_ref, 2 * width + at, temporal)
        mixed = None
        for second in (False, True):
            lanes = head_lanes(rows, second)
            probs = softmax_of(jnp.where(lanes, q, 0), k, allowed).astype(BF16)
            part = dot(probs, jnp.where(lanes, v, 0), NN)
            mixed = part if mixed is None else mixed + part
        put_rows(mix_ref, at, mixed, temporal)


def attend_back_kernel(qkv_ref, mix_g_ref, qkv_g_ref, *, temporal):
    width = mix_g_ref.shape[-1]
    rows = TIMES * 8 if temporal else mix_g_ref.shape[0]
    allowed = same_sequence(rows, temporal)
    scale = HS ** -0.5
    for pair in range(width // (2 * HS)):
        at = pair * 2 * HS
        q = rows_of(qkv_ref, at, temporal)
        k = rows_of(qkv_ref, width + at, temporal)
        v = rows_of(qkv_ref, 2 * width + at, temporal)
        g = rows_of(mix_g_ref, at, temporal)
        total = [None, None, None]
        for second in (False, True):
            lanes = head_lanes(rows, second)
            q_one, g_one = jnp.where(lanes, q, 0), jnp.where(lanes, g, 0)
            probs = softmax_of(q_one, k, allowed)
            prob_g = dot(g_one, v, NT)
            inner = jnp.sum(prob_g * probs, axis=-1, keepdims=True)
            score_g = (probs * (prob_g - inner)).astype(BF16)
            parts = (
                dot(score_g, jnp.where(lanes, k, 0), NN),
                dot(score_g, q_one, TN),
                dot(probs.astype(BF16), g_one, TN),
            )
            total = [p if t is None else t + p for t, p in zip(total, parts)]
        put_rows(qkv_g_ref, at, total[0] * scale, temporal)
        put_rows(qkv_g_ref, width + at, total[1] * scale, temporal)
        put_rows(qkv_g_ref, 2 * width + at, total[2], temporal)


def attention_call(kernel, operands, out_width, temporal):
    total = operands[0].shape[0]
    if temporal:
        seqs = total // TIMES
        grid = (seqs // 8,)

        def spec(cols):
            return pl.BlockSpec((TIMES, 8, cols), lambda i: (0, i, 0))

        operands = [x.reshape(TIMES, seqs, x.shape[-1]) for x in operands]
        out_shape = (TIMES, seqs, out_width)
    else:
        rows = 4 * SLOT
        grid = (total // rows,)

        def spec(cols):
            return pl.BlockSpec((rows, cols), lambda i: (i, 0))

        out_shape = (total, out_width)
    rows = 128 if temporal else 4 * SLOT
    dots = 2 if len(operands) == 1 else 5
    out = pl.pallas_call(
        functools.partial(kernel, temporal=temporal),
        grid=grid,
        in_specs=[spec(x.shape[-1]) for x in operands],
        out_specs=spec(out_width),
        out_shape=jax.ShapeDtypeStruct(out_shape, BF16),
        cost_estimate=pl.CostEstimate(
            flops=dots * grid[0] * 12 * rows * rows * 256,
            bytes_accessed=2 * total * (out_width + sum(x.shape[-1] for x in operands)),
            transcendentals=grid[0] * 12 * rows * rows,
        ),
    )(*operands)
    return out.reshape(total, out_width)


class Copies:
    def __init__(self, send_sems, recv_sems):
        self.send_sems, self.recv_sems, self.made = send_sems, recv_sems, []

    def start(self, source, target, device):
        at = len(self.made)
        copy = pltpu.make_async_remote_copy(
            src_ref=source, dst_ref=target, send_sem=self.send_sems.at[at],
            recv_sem=self.recv_sems.at[at], device_id=device,
            device_id_type=pl.DeviceIdType.MESH,
        )
        copy.start()
        self.made.append(copy)
        return copy


def here():
    a = lax.axis_index("a")
    z = 2 * lax.axis_index("b") + lax.axis_index("c")
    core, x, y = a % 2, (a // 2) % 2, a // 4
    flips = {1: 1 - 2 * core, 2: 2 - 4 * x, 4: 4 - 8 * y, 0: 0}

    def part(mask):
        return a + flips[mask & 1] + flips[mask & 2] + flips[mask & 4]

    return a, z, part


def plane(part, mask):
    return {"a": part(mask)}


def column(z):
    return {"b": z // 2, "c": z % 2}


def greet(part, z):
    barrier = pltpu.get_barrier_semaphore()
    for device in [plane(part, m) for m in (1, 2, 4)] + [column((z + j) % 4) for j in (1, 2, 3)]:
        pl.semaphore_signal(barrier, inc=1, device_id=device, device_id_type=pl.DeviceIdType.MESH)
    pl.semaphore_wait(barrier, 6)


def gather_kernel(*refs, count):
    shards, fulls = refs[:count], refs[count : 2 * count]
    staging = refs[2 * count : 3 * count]
    send_sems, recv_sems, local_sems = refs[3 * count :]
    me, z, part = here()
    loads = [
        pltpu.make_async_copy(shards[w], staging[w], local_sems.at[w]) for w in range(count)
    ]
    for load in loads:
        load.start()
    greet(part, z)
    copies = Copies(send_sems, recv_sems)
    items = []
    for w in range(count):
        for j in (1, 2, 3):
            sent = copies.start(
                shards[w].at[:, me], fulls[w].at[:, z, me], column((z + j) % 4)
            )
            items.append((w, (z + 4 - j) % 4, sent))
    stores = []
    for w in range(count):
        loads[w].wait()
        store = pltpu.make_async_copy(staging[w], fulls[w].at[:, z], local_sems.at[count + w])
        store.start()
        stores.append(store)
    total, lag = len(items), 3
    from_x, from_y, from_far, from_core = {}, {}, {}, []

    def push(w, zz, mask, to):
        at = part(mask)
        return copies.start(fulls[w].at[:, zz, at], fulls[w].at[:, zz, at], plane(part, to))

    for step in range(total + 2 * lag):
        if step < total:
            w, zz, sent = items[step]
            sent.wait_recv()
            from_x[step] = push(w, zz, 0, 2)
            from_y[step] = push(w, zz, 0, 4)
            from_core.append(push(w, zz, 0, 1))
        late = step - lag
        if 0 <= late < total:
            w, zz, _ = items[late]
            from_x[late].wait_recv()
            if late % 2 == 0:
                from_far[late] = push(w, zz, 2, 4)
            from_core.append(push(w, zz, 2, 1))
            from_y[late].wait_recv()
            if late % 2 == 1:
                from_far[late] = push(w, zz, 4, 2)
            from_core.append(push(w, zz, 4, 1))
        last = step - 2 * lag
        if 0 <= last < total:
            w, zz, _ = items[last]
            from_far[last].wait_recv()
            from_core.append(push(w, zz, 6, 1))
    for copy in from_core:
        copy.wait_recv()
    for copy in copies.made:
        copy.wait_send()
    for store in stores:
        store.wait()


def gather_weights(shards, dp, tp):
    count = len(shards)
    views = [x.reshape(x.shape[0], dp, x.shape[1] // dp, x.shape[2]) for x in shards]
    anywhere = pl.BlockSpec(memory_space=pl.ANY)
    sent = sum(x.size for x in shards) * 2
    fulls = pl.pallas_call(
        functools.partial(gather_kernel, count=count),
        out_shape=[
            jax.ShapeDtypeStruct((v.shape[0], tp) + v.shape[1:], v.dtype) for v in views
        ],
        in_specs=[anywhere] * count,
        out_specs=[anywhere] * count,
        scratch_shapes=[pltpu.VMEM(v.shape, v.dtype) for v in views]
        + [
            pltpu.SemaphoreType.DMA((count * 27,)),
            pltpu.SemaphoreType.DMA((count * 27,)),
            pltpu.SemaphoreType.DMA((2 * count,)),
        ],
        compiler_params=pltpu.CompilerParams(collective_id=0, has_side_effects=True),
        cost_estimate=pl.CostEstimate(flops=0, bytes_accessed=40 * sent, transcendentals=0),
        name="gather_weights",
    )(*views)
    return [f.reshape(f.shape[0], -1, f.shape[-1]) for f in fulls]


BLOCKS = (6, 2, 4, 0)


def add_into(target, source):
    def step(i, carry):
        target[i] = (target[i].astype(F32) + source[i].astype(F32)).astype(BF16)
        return carry

    lax.fori_loop(0, target.shape[0], step, 0)


def scatter_kernel(*refs, cuts):
    count = len(cuts)
    held = max(c[0] for c in cuts) + 1
    packs, outs = refs[:held], refs[held : 2 * held]
    refs = refs[2 * held :]
    accs, cores, firsts, seconds, columns = (
        refs[i * count : (i + 1) * count] for i in range(5)
    )
    send_sems, recv_sems, local_sems = refs[5 * count :]
    me, z, part = here()
    near, far = (2, 4), (4, 2)

    def pack_of(s, at):
        w, low, high = cuts[s]
        return packs[w].at[at, :, low:high]

    def out_of(s, at):
        w, low, high = cuts[s]
        return outs[w].at[at, low:high]

    loads = {}
    for s in range(count):
        for b, mask in enumerate(BLOCKS):
            loads[s, b] = pltpu.make_async_copy(
                pack_of(s, part(mask)), accs[s].at[b], local_sems.at[4 * s + b]
            )
            loads[s, b].start()
    greet(part, z)
    copies = Copies(send_sems, recv_sems)
    first_core, hop, lines, along, relays, ends = {}, {}, {}, {}, {}, []
    for g in range(count // 2):
        for b, mask in enumerate(BLOCKS):
            for s in (2 * g, 2 * g + 1):
                first_core[s, b] = copies.start(
                    pack_of(s, part(mask ^ 1)), cores[s].at[b], plane(part, 1)
                )

    def push(s, mask, to):
        at = part(mask)
        return copies.start(out_of(s, at), out_of(s, at), plane(part, to))

    def add_cores(pair):
        for b, mask in enumerate(BLOCKS):
            for s in pair:
                loads[s, b].wait()
                first_core[s, b].wait_recv()
                add_into(accs[s].at[b], cores[s].at[b])
            for s in pair:
                if mask & near[s % 2]:
                    slot = 0 if mask == 6 else 1
                    hop[s, slot] = copies.start(
                        accs[s].at[b], firsts[s].at[slot], plane(part, near[s % 2])
                    )

    def add_first(pair):
        for s in pair:
            hop[s, 0].wait_recv()
            add_into(accs[s].at[BLOCKS.index(far[s % 2])], firsts[s].at[0])
        for s in pair:
            hop[s, 2] = copies.start(
                accs[s].at[BLOCKS.index(far[s % 2])], seconds[s], plane(part, far[s % 2])
            )

    def add_second(pair):
        for s in pair:
            hop[s, 1].wait_recv()
            add_into(accs[s].at[3], firsts[s].at[1])
        for s in pair:
            hop[s, 2].wait_recv()
            add_into(accs[s].at[3], seconds[s])
        for s in pair:
            for j in (1, 2, 3):
                to = (z + j) % 4
                lines[s, j] = copies.start(accs[s].at[3, to], columns[s].at[j - 1], column(to))

    def add_columns(pair):
        for s in pair:
            total = accs[s][3, z].astype(F32)
            for j in (1, 2, 3):
                lines[s, j].wait_recv()
                total = total + columns[s][j - 1].astype(F32)
            w, low, high = cuts[s]
            outs[w][me, low:high] = total.astype(BF16)
        for s in pair:
            along[s, 2] = push(s, 0, 2)
            along[s, 4] = push(s, 0, 4)
            ends.append(push(s, 0, 1))

    def relay(pair):
        for s in pair:
            for mask in (2, 4):
                along[s, mask].wait_recv()
                if mask == near[s % 2]:
                    relays[s] = push(s, mask, far[s % 2])
                ends.append(push(s, mask, 1))

    def finish(pair):
        for s in pair:
            relays[s].wait_recv()
            ends.append(push(s, 6, 1))

    stages = (add_cores, add_first, add_second, add_columns, relay, finish)
    for step in range(count // 2 + len(stages) - 1):
        for i, stage in enumerate(stages):
            if 0 <= step - i < count // 2:
                stage((2 * (step - i), 2 * (step - i) + 1))
    for copy in ends:
        copy.wait_recv()
    for copy in copies.made:
        copy.wait_send()


def scatter_sum(packs):
    cuts = []
    for w, pack in enumerate(packs):
        rows = pack.shape[2]
        half = rows // 32 * 16
        cuts += [(w, 0, half), (w, half, rows)]
    width = packs[0].shape[3]
    anywhere = pl.BlockSpec(memory_space=pl.ANY)

    def scratch(*lead):
        return [pltpu.VMEM(lead + (high - low, width), BF16) for _, low, high in cuts]

    return pl.pallas_call(
        functools.partial(scatter_kernel, cuts=tuple(cuts)),
        out_shape=[jax.ShapeDtypeStruct((8,) + p.shape[2:], BF16) for p in packs],
        in_specs=[anywhere] * len(packs),
        out_specs=[pl.BlockSpec(memory_space=pltpu.VMEM)] * len(packs),
        scratch_shapes=scratch(4, 4) + scratch(4, 4) + scratch(2, 4) + scratch(4) + scratch(3)
        + [
            pltpu.SemaphoreType.DMA((17 * len(cuts),)),
            pltpu.SemaphoreType.DMA((17 * len(cuts),)),
            pltpu.SemaphoreType.DMA((4 * len(cuts),)),
        ],
        compiler_params=pltpu.CompilerParams(collective_id=1, has_side_effects=True),
        cost_estimate=pl.CostEstimate(flops=0, bytes_accessed=300000000, transcendentals=0),
        name="scatter_sum",
    )(*packs)


def build(mesh):
    dp, tp = mesh.shape["dp"], mesh.shape["tensor"]
    count = dp * tp
    groups = count // TIMES
    if groups <= tp:
        shape = (dp, tp // groups, groups)
        names = dict(time=("a", "b"), tensor=("b", "c"), dp=("a",))
    else:
        shape = (TIMES, groups // tp, tp)
        names = dict(time=("a",), tensor=("c",), dp=("a", "b"))
    inner = Mesh(mesh.devices.reshape(shape), ("a", "b", "c"))
    return inner, names, dp, tp


def make_device(names, dp, tp):
    every = ("a", "b", "c")

    def regroup(x):
        return lax.all_to_all(x, names["time"], split_axis=0, concat_axis=0, tiled=True)

    def gather_all(piece):
        full = lax.all_gather(piece, every, axis=0, tiled=False)
        return full.reshape((dp, tp) + piece.shape)

    def per_device(
        tokens, space_gain, space_shift, space_inproj, space_bias, space_outproj,
        space_outbias, time_gain, time_shift, time_inproj, time_bias, time_outproj,
        time_outbias, feed_gain, feed_shift, up_weight, up_bias, down_weight,
        down_bias, cotangent,
    ):
        width = tokens.shape[-1]
        own = tokens.shape[0] * tokens.shape[1]
        heads_width = space_inproj.shape[2]
        units = up_weight.shape[0]
        d_index = lax.axis_index(names["dp"])
        k_index = lax.axis_index(names["tensor"])
        hp, up = heads_width // dp, units // dp

        def piece_of(rows, per):
            return lax.dynamic_slice_in_dim(rows, d_index * per, per, rows.ndim - 2)

        def attn_piece(inproj, outproj):
            in_piece = piece_of(inproj.transpose(1, 2, 0), hp).reshape(3 * hp, width)
            return jnp.concatenate([in_piece, piece_of(outproj, hp)], axis=0)

        def attn_full(full):
            w_in = full[:, :, : 3 * hp].reshape(dp, tp, 3, hp, width)
            w_in = w_in.transpose(2, 1, 0, 3, 4).reshape(3 * width, width)
            w_out = full[:, :, 3 * hp : 4 * hp].transpose(1, 0, 2, 3).reshape(width, width)
            return w_in, w_out

        def in_rows(inproj):
            return inproj.transpose(1, 2, 0)

        direct = (dp, tp) == (8, 4)
        bias_shard = jnp.concatenate([up_bias, space_bias.reshape(-1), time_bias.reshape(-1)])
        per_row = bias_shard.shape[0] // dp
        if direct:
            bias_rows = jnp.pad(
                bias_shard.reshape(dp, 1, per_row), ((0, 0), (0, 7), (0, width - per_row))
            )
            space_in_w, space_out_w, time_in_w, time_out_w, bias_full = [
                w.reshape(-1, width)
                for w in gather_weights(
                    [
                        in_rows(space_inproj), space_outproj[None], in_rows(time_inproj),
                        time_outproj[None], bias_rows.reshape(1, -1, width),
                    ],
                    dp, tp,
                )
            ]
            biases = bias_full.reshape(tp, dp, 8, width)[:, :, 0, :per_row].reshape(tp, -1)
        else:
            space_in_w, space_out_w = attn_full(gather_all(attn_piece(space_inproj, space_outproj)))
            time_in_w, time_out_w = attn_full(gather_all(attn_piece(time_inproj, time_outproj)))
            biases = lax.all_gather(bias_shard, names["tensor"], axis=0, tiled=False)
        biases = biases.astype(F32)
        full_feed = gather_all(
            jnp.concatenate([piece_of(up_weight, up), piece_of(down_weight, up)], axis=0)
        )
        up_w = full_feed[:, :, :up].reshape(dp * tp * up, width)
        down_w = full_feed[:, :, up:].reshape(dp * tp * up, width)
        up_b = biases[:, :units].reshape(tp, dp, up).transpose(1, 0, 2).reshape(-1)

        def in_bias(start):
            pair = biases[:, start : start + 2 * heads_width].reshape(tp, 2, heads_width)
            pair = pair.transpose(1, 0, 2).reshape(2, width)
            return jnp.concatenate([pair[0], jnp.zeros((width,), F32), pair[1]])

        space_b, time_b = in_bias(units), in_bias(units + 2 * heads_width)

        seqs = own // TIMES
        slots = TIMES * SLOT

        def pad_rows(x):
            x = x.reshape(TIMES, seqs, width)
            return jnp.pad(x, ((0, 0), (0, SLOT - seqs), (0, 0))).reshape(slots, width)

        def unpad(x):
            return x.reshape(TIMES, SLOT, width)[:, :seqs].reshape(tokens.shape)

        def exchange(x):
            return regroup(x.reshape(TIMES, SLOT, width)).reshape(slots, width)

        cot_slots = pad_rows(cotangent)

        resid = pad_rows(tokens).astype(F32)
        space_n, space_r = norm_stats(resid)
        space_in = (space_n * space_gain + space_shift).astype(BF16)
        space_qkv = (dot(space_in, space_in_w, NT) + space_b).astype(BF16)
        space_mix = attention_call(attend_kernel, [space_qkv], width, False)
        after_space = resid + dot(space_mix, space_out_w, NN) + space_outbias.astype(F32)

        moved = exchange(after_space.astype(BF16))
        moved, up_w, down_w, cot_slots = lax.optimization_barrier((moved, up_w, down_w, cot_slots))
        cot = exchange(cot_slots)
        after_space_p = moved.astype(F32)
        tn_p, tr_p = norm_stats(after_space_p)
        time_in = (tn_p * time_gain + time_shift).astype(BF16)
        time_qkv = (dot(time_in, time_in_w, NT) + time_b).astype(BF16)
        time_mix = attention_call(attend_kernel, [time_qkv], width, True)
        after_time = after_space_p + dot(time_mix, time_out_w, NN) + time_outbias.astype(F32)
        feed_n, feed_r = norm_stats(after_time)
        feed_in = (feed_n * feed_gain + feed_shift).astype(BF16)
        pre = dot(feed_in, up_w, NT) + up_b
        hidden = gelu_exact(pre).astype(BF16)
        layer_p = (after_time + dot(hidden, down_w, NN) + down_bias.astype(F32)).astype(BF16)
        layer_out = unpad(exchange(layer_p))

        upstream = cot.astype(F32)
        down_bias_g = jnp.sum(upstream, axis=0)
        down_g = dot(hidden, cot, TN).astype(BF16)
        pre_g = (dot(cot, down_w, NT) * gelu_slope(pre)).astype(BF16)
        up_g = dot(pre_g, feed_in, TN).astype(BF16)
        up_bias_g = jnp.sum(pre_g.astype(F32), axis=0)
        feed_g = dot(pre_g, up_w, NN)
        feed_gain_g = jnp.sum(feed_g * feed_n, axis=0)
        feed_shift_g = jnp.sum(feed_g, axis=0)
        after_time_g = upstream + norm_back(feed_g, feed_n, feed_r, feed_gain)

        def scatter(grad):
            return lax.psum_scatter(grad, every, scatter_dimension=0, tiled=False)

        feed_pack = jnp.concatenate(
            [up_g.reshape(dp * tp, up, width), down_g.reshape(dp * tp, up, width)], axis=1
        )
        feed_pack, after_time_g = lax.optimization_barrier((feed_pack, after_time_g))
        feed_part = scatter(feed_pack)

        def attention_back(branch, normed_in, qkv, mix, w_in, w_out, temporal):
            outbias_g = jnp.sum(branch.astype(F32), axis=0)
            mix_g = dot(branch, w_out, NT).astype(BF16)
            qkv_g = attention_call(attend_back_kernel, [qkv, mix_g], 3 * width, temporal)
            normed_g = dot(qkv_g, w_in, NN)
            return normed_g, qkv_g, outbias_g

        def attention_weights(branch, normed_in, mix, qkv_g):
            sums = jnp.sum(qkv_g.astype(F32), axis=0).reshape(3, width)
            out_g = dot(mix, branch, TN).astype(BF16)
            in_g = dot(qkv_g, normed_in, TN).astype(BF16)
            pack = jnp.concatenate(
                [
                    in_g.reshape(3, tp, dp, hp, width)
                    .transpose(2, 1, 0, 3, 4)
                    .reshape(dp * tp, 3 * hp, width),
                    out_g.reshape(tp, dp, hp, width)
                    .transpose(1, 0, 2, 3)
                    .reshape(dp * tp, hp, width),
                ],
                axis=1,
            )
            return pack, sums

        time_branch = after_time_g.astype(BF16)
        time_in_g, time_qkv_g, time_outbias_g = attention_back(
            time_branch, time_in, time_qkv, time_mix, time_in_w, time_out_w, True
        )
        time_gain_g = jnp.sum(time_in_g * tn_p, axis=0)
        time_shift_g = jnp.sum(time_in_g, axis=0)
        after_space_g_p = after_time_g + norm_back(time_in_g, tn_p, tr_p, time_gain)

        high = exchange(after_space_g_p.astype(BF16))
        time_pack, time_sums = attention_weights(time_branch, time_in, time_mix, time_qkv_g)
        after_space_g = high.astype(F32)

        space_in_g, space_qkv_g, space_outbias_g = attention_back(
            high, space_in, space_qkv, space_mix, space_in_w, space_out_w, False
        )
        space_pack, space_sums = attention_weights(high, space_in, space_mix, space_qkv_g)
        space_gain_g = jnp.sum(space_in_g * space_n, axis=0)
        space_shift_g = jnp.sum(space_in_g, axis=0)
        input_g = unpad(after_space_g + norm_back(space_in_g, space_n, space_r, space_gain))

        shared = jnp.concatenate(
            [
                space_gain_g, space_shift_g, space_outbias_g, time_gain_g, time_shift_g,
                time_outbias_g, feed_gain_g, feed_shift_g, down_bias_g,
            ]
        )
        headed = jnp.stack([space_sums[0], space_sums[2], time_sums[0], time_sums[2]])
        headed = headed.reshape(4, tp, heads_width).transpose(1, 0, 2).reshape(tp, -1)
        upped = up_bias_g.reshape(dp, tp, up).transpose(1, 0, 2).reshape(tp, -1)
        sharded = jnp.concatenate([headed, upped], axis=1)
        many, few = 9 * width // dp, sharded.shape[1] // dp
        small = jnp.concatenate(
            [
                jnp.broadcast_to(shared.reshape(dp, 1, many), (dp, tp, many)),
                sharded.reshape(tp, dp, few).transpose(1, 0, 2),
                jnp.zeros((dp, tp, 2 * width - many - few), F32),
            ],
            axis=2,
        ).astype(BF16)
        small = jnp.pad(small.reshape(dp * tp, 2, width), ((0, 0), (0, 14), (0, 0)))
        space_pack = jnp.concatenate([space_pack, small], axis=1)

        def spread(part):
            return lax.all_gather(part, names["dp"], axis=0, tiled=False)

        if direct:
            time_all, space_all = scatter_sum(
                [x.reshape((dp, tp, -1, width)) for x in (time_pack, space_pack)]
            )
        else:
            both = spread(scatter(jnp.concatenate([time_pack, space_pack], axis=1)))
            time_all, space_all = both[:, : 4 * hp], both[:, 4 * hp :]

        def attn_out(full):
            in_out = full[:, : 3 * hp].reshape(dp, 3, hp, width).transpose(1, 0, 2, 3)
            in_out = in_out.reshape(3, heads_width, width).transpose(2, 0, 1).astype(F32)
            return in_out, full[:, 3 * hp : 4 * hp].reshape(heads_width, width).astype(F32)

        feed_all = spread(feed_part)
        time_in_out, time_out_out = attn_out(time_all)
        space_in_out, space_out_out = attn_out(space_all)
        sums = space_all[:, 4 * hp : 4 * hp + 2].reshape(dp, 2 * width).astype(F32)
        rows = sums[:, :many].reshape(9, width)
        own_sums = sums[:, many : many + few].reshape(-1)
        head_rows = own_sums[: 4 * heads_width].reshape(4, heads_width)
        up_bias_out = own_sums[4 * heads_width :]
        return (
            layer_out,
            input_g,
            rows[0], rows[1], space_in_out, head_rows[0:2], space_out_out, rows[2],
            rows[3], rows[4], time_in_out, head_rows[2:4], time_out_out, rows[5],
            rows[6], rows[7],
            feed_all[:, :up].reshape(units, width).astype(F32),
            up_bias_out,
            feed_all[:, up:].reshape(units, width).astype(F32),
            rows[8],
        )

    return per_device


def solution(mesh):
    inner, names, dp, tp = build(mesh)
    every, tensor = ("a", "b", "c"), names["tensor"]
    frames = P(every, None, None)
    head_in = P(None, None, tensor)
    head_bias = P(None, tensor)
    row = P(tensor, None)
    return jax.shard_map(
        make_device(names, dp, tp),
        mesh=inner,
        in_specs=(
            frames, P(), P(), head_in, head_bias, row, P(),
            P(), P(), head_in, head_bias, row, P(),
            P(), P(), row, P(tensor), row, P(), frames,
        ),
        out_specs=(
            frames, frames, P(), P(), head_in, head_bias, row, P(),
            P(), P(), head_in, head_bias, row, P(),
            P(), P(), row, P(tensor), row, P(),
        ),
        check_vma=False,
    )
```

```python
import functools

import jax
import jax.numpy as jnp
from jax import lax
from jax.experimental import pallas as pl
from jax.experimental.pallas import tpu as pltpu
from jax.sharding import Mesh, PartitionSpec as P

HS = 64
PATCH = 196
TIMES = 16
SLOT = 56
UNROLL = 6
EPSILON = 1e-06
ROOT_HALF = 0.7071067811865476
INV_ROOT_TAU = 0.3989422804014327
F32 = jnp.float32
BF16 = jnp.bfloat16
NT = (((1,), (1,)), ((), ()))
NN = (((1,), (0,)), ((), ()))
TN = (((0,), (0,)), ((), ()))


def dot(a, b, dims):
    return lax.dot_general(a, b, dims, preferred_element_type=F32)


def norm_stats(values):
    center = values - jnp.mean(values, axis=-1, keepdims=True)
    second = jnp.mean(center * center, axis=-1, keepdims=True)
    rate = lax.rsqrt(second + EPSILON)
    return center * rate, rate


def norm_back(grad, normed, rate, gain):
    e = grad * gain
    inner = jnp.mean(e * normed, axis=-1, keepdims=True)
    return rate * (e - jnp.mean(e, axis=-1, keepdims=True) - normed * inner)


def gelu_exact(values):
    return 0.5 * values * (1.0 + lax.erf(values * ROOT_HALF))


def gelu_slope(values):
    return (
        0.5 * (1.0 + lax.erf(values * ROOT_HALF))
        + values * jnp.exp(-0.5 * values * values) * INV_ROOT_TAU
    )


def same_sequence(rows, temporal):
    r = lax.broadcasted_iota(jnp.int32, (rows, rows), 0)
    c = lax.broadcasted_iota(jnp.int32, (rows, rows), 1)
    if temporal:
        return (r % 8) == (c % 8)
    return (c % SLOT) < (PATCH // 4)


def head_lanes(rows, second):
    lane = lax.broadcasted_iota(jnp.int32, (rows, 2 * HS), 1)
    return (lane >= HS) if second else (lane < HS)


def softmax_of(q_one, k_pair, allowed):
    scores = jnp.where(allowed, dot(q_one, k_pair, NT), -1e30)
    top = jnp.max(scores, axis=-1, keepdims=True)
    weights = jnp.exp(scores - top)
    return weights * (1.0 / jnp.sum(weights, axis=-1, keepdims=True))


def rows_of(ref, start, temporal):
    if temporal:
        block = ref[:, :, pl.ds(start, 2 * HS)].astype(F32)
        return block.reshape(-1, 2 * HS).astype(BF16)
    return ref[:, pl.ds(start, 2 * HS)]


def put_rows(ref, start, value, temporal):
    if temporal:
        ref[:, :, pl.ds(start, 2 * HS)] = value.reshape(TIMES, 8, 2 * HS).astype(BF16)
    else:
        ref[:, pl.ds(start, 2 * HS)] = value.astype(BF16)


def over_pairs(width, body):
    def step(pair, carry):
        body(pl.multiple_of(pair * 2 * HS, 2 * HS))
        return carry

    lax.fori_loop(0, width // (2 * HS), step, 0, unroll=UNROLL)


def attend_kernel(qkv_ref, mix_ref, *, temporal):
    width = mix_ref.shape[-1]
    rows = TIMES * 8 if temporal else mix_ref.shape[0]
    allowed = same_sequence(rows, temporal)

    def one_pair(at):
        q = rows_of(qkv_ref, at, temporal) * jnp.asarray(HS ** -0.5, BF16)
        k = rows_of(qkv_ref, width + at, temporal)
        v = rows_of(qkv_ref, 2 * width + at, temporal)
        mixed = None
        for second in (False, True):
            lanes = head_lanes(rows, second)
            probs = softmax_of(jnp.where(lanes, q, 0), k, allowed).astype(BF16)
            part = dot(probs, jnp.where(lanes, v, 0), NN)
            mixed = part if mixed is None else mixed + part
        put_rows(mix_ref, at, mixed, temporal)

    over_pairs(width, one_pair)


def attend_back_kernel(qkv_ref, mix_g_ref, qkv_g_ref, *, temporal):
    width = mix_g_ref.shape[-1]
    rows = TIMES * 8 if temporal else mix_g_ref.shape[0]
    allowed = same_sequence(rows, temporal)
    scale = HS ** -0.5

    def one_pair(at):
        q = rows_of(qkv_ref, at, temporal) * jnp.asarray(HS ** -0.5, BF16)
        k = rows_of(qkv_ref, width + at, temporal)
        v = rows_of(qkv_ref, 2 * width + at, temporal)
        g = rows_of(mix_g_ref, at, temporal)
        total = [None, None, None]
        for second in (False, True):
            lanes = head_lanes(rows, second)
            q_one, g_one = jnp.where(lanes, q, 0), jnp.where(lanes, g, 0)
            probs = softmax_of(q_one, k, allowed)
            prob_g = dot(g_one, v, NT)
            inner = jnp.sum(prob_g * probs, axis=-1, keepdims=True)
            score_g = (probs * (prob_g - inner)).astype(BF16)
            parts = (
                dot(score_g, jnp.where(lanes, k, 0), NN),
                dot(score_g, q_one, TN),
                dot(probs.astype(BF16), g_one, TN),
            )
            total = [p if t is None else t + p for t, p in zip(total, parts)]
        put_rows(qkv_g_ref, at, total[0] * scale, temporal)
        put_rows(qkv_g_ref, width + at, total[1], temporal)
        put_rows(qkv_g_ref, 2 * width + at, total[2], temporal)

    over_pairs(width, one_pair)


def attention_call(kernel, operands, out_width, temporal):
    total = operands[0].shape[0]
    if temporal:
        seqs = total // TIMES
        grid = (seqs // 8,)

        def spec(cols):
            return pl.BlockSpec((TIMES, 8, cols), lambda i: (0, i, 0))

        operands = [x.reshape(TIMES, seqs, x.shape[-1]) for x in operands]
        out_shape = (TIMES, seqs, out_width)
    else:
        rows = 4 * SLOT
        grid = (total // rows,)

        def spec(cols):
            return pl.BlockSpec((rows, cols), lambda i: (i, 0))

        out_shape = (total, out_width)
    rows = 128 if temporal else 4 * SLOT
    dots = 2 if len(operands) == 1 else 5
    out = pl.pallas_call(
        functools.partial(kernel, temporal=temporal),
        grid=grid,
        in_specs=[spec(x.shape[-1]) for x in operands],
        out_specs=spec(out_width),
        out_shape=jax.ShapeDtypeStruct(out_shape, BF16),
        cost_estimate=pl.CostEstimate(
            flops=dots * grid[0] * 12 * rows * rows * 256,
            bytes_accessed=2 * total * (out_width + sum(x.shape[-1] for x in operands)),
            transcendentals=grid[0] * 12 * rows * rows,
        ),
    )(*operands)
    return out.reshape(total, out_width)


class Copies:
    def __init__(self, send_sems, recv_sems):
        self.send_sems, self.recv_sems, self.made = send_sems, recv_sems, []

    def start(self, source, target, device):
        at = len(self.made)
        copy = pltpu.make_async_remote_copy(
            src_ref=source, dst_ref=target, send_sem=self.send_sems.at[at],
            recv_sem=self.recv_sems.at[at], device_id=device,
            device_id_type=pl.DeviceIdType.MESH,
        )
        copy.start()
        self.made.append(copy)
        return copy


def here():
    a = lax.axis_index("a")
    z = 2 * lax.axis_index("b") + lax.axis_index("c")
    core, x, y = a % 2, (a // 2) % 2, a // 4
    flips = {1: 1 - 2 * core, 2: 2 - 4 * x, 4: 4 - 8 * y, 0: 0}

    def part(mask):
        return a + flips[mask & 1] + flips[mask & 2] + flips[mask & 4]

    return a, z, part


def plane(part, mask):
    return {"a": part(mask)}


def column(z):
    return {"b": z // 2, "c": z % 2}


def greet(part, z):
    barrier = pltpu.get_barrier_semaphore()
    for device in [plane(part, m) for m in (1, 2, 4)] + [column((z + j) % 4) for j in (1, 2, 3)]:
        pl.semaphore_signal(barrier, inc=1, device_id=device, device_id_type=pl.DeviceIdType.MESH)
    pl.semaphore_wait(barrier, 6)


def gather_kernel(*refs, count):
    shards, fulls = refs[:count], refs[count : 2 * count]
    staging = refs[2 * count : 3 * count]
    send_sems, recv_sems, local_sems = refs[3 * count :]
    me, z, part = here()
    loads = [
        pltpu.make_async_copy(shards[w], staging[w], local_sems.at[w]) for w in range(count)
    ]
    for load in loads:
        load.start()
    greet(part, z)
    copies = Copies(send_sems, recv_sems)
    items = []
    for w in range(count):
        for j in (1, 2, 3):
            sent = copies.start(
                shards[w].at[:, me], fulls[w].at[:, z, me], column((z + j) % 4)
            )
            items.append((w, (z + 4 - j) % 4, sent))
    stores = []
    for w in range(count):
        loads[w].wait()
        store = pltpu.make_async_copy(staging[w], fulls[w].at[:, z], local_sems.at[count + w])
        store.start()
        stores.append(store)
    total, lag = len(items), 3
    from_x, from_y, from_far, from_core = {}, {}, {}, []

    def push(w, zz, mask, to):
        at = part(mask)
        return copies.start(fulls[w].at[:, zz, at], fulls[w].at[:, zz, at], plane(part, to))

    for step in range(total + 2 * lag):
        if step < total:
            w, zz, sent = items[step]
            sent.wait_recv()
            from_x[step] = push(w, zz, 0, 2)
            from_y[step] = push(w, zz, 0, 4)
            from_core.append(push(w, zz, 0, 1))
        late = step - lag
        if 0 <= late < total:
            w, zz, _ = items[late]
            from_x[late].wait_recv()
            if late % 2 == 0:
                from_far[late] = push(w, zz, 2, 4)
            from_core.append(push(w, zz, 2, 1))
            from_y[late].wait_recv()
            if late % 2 == 1:
                from_far[late] = push(w, zz, 4, 2)
            from_core.append(push(w, zz, 4, 1))
        last = step - 2 * lag
        if 0 <= last < total:
            w, zz, _ = items[last]
            from_far[last].wait_recv()
            from_core.append(push(w, zz, 6, 1))
    for copy in from_core:
        copy.wait_recv()
    for copy in copies.made:
        copy.wait_send()
    for store in stores:
        store.wait()


def gather_weights(shards, dp, tp):
    count = len(shards)
    views = [x.reshape(x.shape[0], dp, x.shape[1] // dp, x.shape[2]) for x in shards]
    anywhere = pl.BlockSpec(memory_space=pl.ANY)
    sent = sum(x.size for x in shards) * 2
    fulls = pl.pallas_call(
        functools.partial(gather_kernel, count=count),
        out_shape=[
            jax.ShapeDtypeStruct((v.shape[0], tp) + v.shape[1:], v.dtype) for v in views
        ],
        in_specs=[anywhere] * count,
        out_specs=[anywhere] * count,
        scratch_shapes=[pltpu.VMEM(v.shape, v.dtype) for v in views]
        + [
            pltpu.SemaphoreType.DMA((count * 27,)),
            pltpu.SemaphoreType.DMA((count * 27,)),
            pltpu.SemaphoreType.DMA((2 * count,)),
        ],
        compiler_params=pltpu.CompilerParams(collective_id=0, has_side_effects=True),
        cost_estimate=pl.CostEstimate(flops=0, bytes_accessed=40 * sent, transcendentals=0),
        name="gather_weights",
    )(*views)
    return [f.reshape(f.shape[0], -1, f.shape[-1]) for f in fulls]


BLOCKS = (6, 2, 4, 0)


def add_into(target, source):
    def step(i, carry):
        target[i] = (target[i].astype(F32) + source[i].astype(F32)).astype(BF16)
        return carry

    lax.fori_loop(0, target.shape[0], step, 0)


def scatter_kernel(*refs, cuts):
    count = len(cuts)
    held = max(c[0] for c in cuts) + 1
    packs, outs = refs[:held], refs[held : 2 * held]
    refs = refs[2 * held :]
    accs, cores, firsts, seconds, columns = (
        refs[i * count : (i + 1) * count] for i in range(5)
    )
    send_sems, recv_sems, local_sems = refs[5 * count :]
    me, z, part = here()
    near, far = (2, 4), (4, 2)

    def pack_of(s, at):
        w, low, high = cuts[s]
        return packs[w].at[at, :, low:high]

    def out_of(s, at):
        w, low, high = cuts[s]
        return outs[w].at[at, low:high]

    loads = {}
    for s in range(count):
        for b, mask in enumerate(BLOCKS):
            loads[s, b] = pltpu.make_async_copy(
                pack_of(s, part(mask)), accs[s].at[b], local_sems.at[4 * s + b]
            )
            loads[s, b].start()
    greet(part, z)
    copies = Copies(send_sems, recv_sems)
    first_core, hop, lines, along, relays, ends = {}, {}, {}, {}, {}, []
    for g in range(count // 2):
        for b, mask in enumerate(BLOCKS):
            for s in (2 * g, 2 * g + 1):
                first_core[s, b] = copies.start(
                    pack_of(s, part(mask ^ 1)), cores[s].at[b], plane(part, 1)
                )

    def push(s, mask, to):
        at = part(mask)
        return copies.start(out_of(s, at), out_of(s, at), plane(part, to))

    def add_cores(pair):
        for b, mask in enumerate(BLOCKS):
            for s in pair:
                loads[s, b].wait()
                first_core[s, b].wait_recv()
                add_into(accs[s].at[b], cores[s].at[b])
            for s in pair:
                if mask & near[s % 2]:
                    slot = 0 if mask == 6 else 1
                    hop[s, slot] = copies.start(
                        accs[s].at[b], firsts[s].at[slot], plane(part, near[s % 2])
                    )

    def add_first(pair):
        for s in pair:
            hop[s, 0].wait_recv()
            add_into(accs[s].at[BLOCKS.index(far[s % 2])], firsts[s].at[0])
        for s in pair:
            hop[s, 2] = copies.start(
                accs[s].at[BLOCKS.index(far[s % 2])], seconds[s], plane(part, far[s % 2])
            )

    def add_second(pair):
        for s in pair:
            hop[s, 1].wait_recv()
            add_into(accs[s].at[3], firsts[s].at[1])
        for s in pair:
            hop[s, 2].wait_recv()
            add_into(accs[s].at[3], seconds[s])
        for s in pair:
            for j in (1, 2, 3):
                to = (z + j) % 4
                lines[s, j] = copies.start(accs[s].at[3, to], columns[s].at[j - 1], column(to))

    def add_columns(pair):
        for s in pair:
            total = accs[s][3, z].astype(F32)
            for j in (1, 2, 3):
                lines[s, j].wait_recv()
                total = total + columns[s][j - 1].astype(F32)
            w, low, high = cuts[s]
            outs[w][me, low:high] = total.astype(BF16)
        for s in pair:
            along[s, 2] = push(s, 0, 2)
            along[s, 4] = push(s, 0, 4)
            ends.append(push(s, 0, 1))

    def relay(pair):
        for s in pair:
            for mask in (2, 4):
                along[s, mask].wait_recv()
                if mask == near[s % 2]:
                    relays[s] = push(s, mask, far[s % 2])
                ends.append(push(s, mask, 1))

    def finish(pair):
        for s in pair:
            relays[s].wait_recv()
            ends.append(push(s, 6, 1))

    stages = (add_cores, add_first, add_second, add_columns, relay, finish)
    for step in range(count // 2 + len(stages) - 1):
        for i, stage in enumerate(stages):
            if 0 <= step - i < count // 2:
                stage((2 * (step - i), 2 * (step - i) + 1))
    for copy in ends:
        copy.wait_recv()
    for copy in copies.made:
        copy.wait_send()


def scatter_sum(packs):
    cuts = []
    for w, pack in enumerate(packs):
        rows = pack.shape[2]
        half = rows // 32 * 16
        cuts += [(w, 0, half), (w, half, rows)]
    width = packs[0].shape[3]
    anywhere = pl.BlockSpec(memory_space=pl.ANY)

    def scratch(*lead):
        return [pltpu.VMEM(lead + (high - low, width), BF16) for _, low, high in cuts]

    return pl.pallas_call(
        functools.partial(scatter_kernel, cuts=tuple(cuts)),
        out_shape=[jax.ShapeDtypeStruct((8,) + p.shape[2:], BF16) for p in packs],
        in_specs=[anywhere] * len(packs),
        out_specs=[pl.BlockSpec(memory_space=pltpu.VMEM)] * len(packs),
        scratch_shapes=scratch(4, 4) + scratch(4, 4) + scratch(2, 4) + scratch(4) + scratch(3)
        + [
            pltpu.SemaphoreType.DMA((17 * len(cuts),)),
            pltpu.SemaphoreType.DMA((17 * len(cuts),)),
            pltpu.SemaphoreType.DMA((4 * len(cuts),)),
        ],
        compiler_params=pltpu.CompilerParams(collective_id=1, has_side_effects=True),
        cost_estimate=pl.CostEstimate(flops=0, bytes_accessed=300000000, transcendentals=0),
        name="scatter_sum",
    )(*packs)


def build(mesh):
    dp, tp = mesh.shape["dp"], mesh.shape["tensor"]
    count = dp * tp
    groups = count // TIMES
    if groups <= tp:
        shape = (dp, tp // groups, groups)
        names = dict(time=("a", "b"), tensor=("b", "c"), dp=("a",))
    else:
        shape = (TIMES, groups // tp, tp)
        names = dict(time=("a",), tensor=("c",), dp=("a", "b"))
    inner = Mesh(mesh.devices.reshape(shape), ("a", "b", "c"))
    return inner, names, dp, tp


def make_device(names, dp, tp):
    every = ("a", "b", "c")

    def regroup(x):
        return lax.all_to_all(x, names["time"], split_axis=0, concat_axis=0, tiled=True)

    def gather_all(piece):
        full = lax.all_gather(piece, every, axis=0, tiled=False)
        return full.reshape((dp, tp) + piece.shape)

    def per_device(
        tokens, space_gain, space_shift, space_inproj, space_bias, space_outproj,
        space_outbias, time_gain, time_shift, time_inproj, time_bias, time_outproj,
        time_outbias, feed_gain, feed_shift, up_weight, up_bias, down_weight,
        down_bias, cotangent,
    ):
        width = tokens.shape[-1]
        own = tokens.shape[0] * tokens.shape[1]
        heads_width = space_inproj.shape[2]
        units = up_weight.shape[0]
        d_index = lax.axis_index(names["dp"])
        k_index = lax.axis_index(names["tensor"])
        hp, up = heads_width // dp, units // dp

        def piece_of(rows, per):
            return lax.dynamic_slice_in_dim(rows, d_index * per, per, rows.ndim - 2)

        def attn_piece(inproj, outproj):
            in_piece = piece_of(inproj.transpose(1, 2, 0), hp).reshape(3 * hp, width)
            return jnp.concatenate([in_piece, piece_of(outproj, hp)], axis=0)

        def attn_full(full):
            w_in = full[:, :, : 3 * hp].reshape(dp, tp, 3, hp, width)
            w_in = w_in.transpose(2, 1, 0, 3, 4).reshape(3 * width, width)
            w_out = full[:, :, 3 * hp : 4 * hp].transpose(1, 0, 2, 3).reshape(width, width)
            return w_in, w_out

        def in_rows(inproj):
            return inproj.transpose(1, 2, 0)

        direct = (dp, tp) == (8, 4)
        bias_shard = jnp.concatenate([up_bias, space_bias.reshape(-1), time_bias.reshape(-1)])
        per_row = bias_shard.shape[0] // dp
        if direct:
            bias_rows = jnp.pad(
                bias_shard.reshape(dp, 1, per_row), ((0, 0), (0, 7), (0, width - per_row))
            )
            space_in_w, space_out_w, time_in_w, time_out_w, bias_full = [
                w.reshape(-1, width)
                for w in gather_weights(
                    [
                        in_rows(space_inproj), space_outproj[None], in_rows(time_inproj),
                        time_outproj[None], bias_rows.reshape(1, -1, width),
                    ],
                    dp, tp,
                )
            ]
            biases = bias_full.reshape(tp, dp, 8, width)[:, :, 0, :per_row].reshape(tp, -1)
        else:
            space_in_w, space_out_w = attn_full(gather_all(attn_piece(space_inproj, space_outproj)))
            time_in_w, time_out_w = attn_full(gather_all(attn_piece(time_inproj, time_outproj)))
            biases = lax.all_gather(bias_shard, names["tensor"], axis=0, tiled=False)
        biases = biases.astype(F32)
        full_feed = gather_all(
            jnp.concatenate([piece_of(up_weight, up), piece_of(down_weight, up)], axis=0)
        )
        up_w = full_feed[:, :, :up].reshape(dp * tp * up, width)
        down_w = full_feed[:, :, up:].reshape(dp * tp * up, width)
        up_b = biases[:, :units].reshape(tp, dp, up).transpose(1, 0, 2).reshape(-1)

        def in_bias(start):
            pair = biases[:, start : start + 2 * heads_width].reshape(tp, 2, heads_width)
            pair = pair.transpose(1, 0, 2).reshape(2, width)
            return jnp.concatenate([pair[0], jnp.zeros((width,), F32), pair[1]])

        space_b, time_b = in_bias(units), in_bias(units + 2 * heads_width)

        seqs = own // TIMES
        slots = TIMES * SLOT

        def pad_rows(x):
            x = x.reshape(TIMES, seqs, width)
            return jnp.pad(x, ((0, 0), (0, SLOT - seqs), (0, 0))).reshape(slots, width)

        def unpad(x):
            return x.reshape(TIMES, SLOT, width)[:, :seqs].reshape(tokens.shape)

        def exchange(x):
            return regroup(x.reshape(TIMES, SLOT, width)).reshape(slots, width)

        cot_slots = pad_rows(cotangent)

        resid = pad_rows(tokens).astype(F32)
        space_n, space_r = norm_stats(resid)
        space_in = (space_n * space_gain + space_shift).astype(BF16)
        space_qkv = (dot(space_in, space_in_w, NT) + space_b).astype(BF16)
        space_mix = attention_call(attend_kernel, [space_qkv], width, False)
        after_space = resid + dot(space_mix, space_out_w, NN) + space_outbias.astype(F32)

        moved = exchange(after_space.astype(BF16))
        moved, up_w, down_w, cot_slots = lax.optimization_barrier((moved, up_w, down_w, cot_slots))
        cot = exchange(cot_slots)
        after_space_p = moved.astype(F32)
        tn_p, tr_p = norm_stats(after_space_p)
        time_in = (tn_p * time_gain + time_shift).astype(BF16)
        time_qkv = (dot(time_in, time_in_w, NT) + time_b).astype(BF16)
        time_mix = attention_call(attend_kernel, [time_qkv], width, True)
        after_time = after_space_p + dot(time_mix, time_out_w, NN) + time_outbias.astype(F32)
        feed_n, feed_r = norm_stats(after_time)
        feed_in = (feed_n * feed_gain + feed_shift).astype(BF16)
        pre = dot(feed_in, up_w, NT) + up_b
        hidden = gelu_exact(pre).astype(BF16)
        layer_p = (after_time + dot(hidden, down_w, NN) + down_bias.astype(F32)).astype(BF16)
        layer_out = unpad(exchange(layer_p))

        upstream = cot.astype(F32)
        down_bias_g = jnp.sum(upstream, axis=0)
        down_g = dot(hidden, cot, TN).astype(BF16)
        pre_g = (dot(cot, down_w, NT) * gelu_slope(pre)).astype(BF16)
        up_g = dot(pre_g, feed_in, TN).astype(BF16)
        up_bias_g = jnp.sum(pre_g.astype(F32), axis=0)
        feed_g = dot(pre_g, up_w, NN)
        feed_gain_g = jnp.sum(feed_g * feed_n, axis=0)
        feed_shift_g = jnp.sum(feed_g, axis=0)
        after_time_g = upstream + norm_back(feed_g, feed_n, feed_r, feed_gain)

        def scatter(grad):
            return lax.psum_scatter(grad, every, scatter_dimension=0, tiled=False)

        feed_pack = jnp.concatenate(
            [up_g.reshape(dp * tp, up, width), down_g.reshape(dp * tp, up, width)], axis=1
        )
        feed_pack, after_time_g = lax.optimization_barrier((feed_pack, after_time_g))
        feed_part = scatter(feed_pack)

        def attention_back(branch, normed_in, qkv, mix, w_in, w_out, temporal):
            outbias_g = jnp.sum(branch.astype(F32), axis=0)
            mix_g = dot(branch, w_out, NT).astype(BF16)
            qkv_g = attention_call(attend_back_kernel, [qkv, mix_g], 3 * width, temporal)
            normed_g = dot(qkv_g, w_in, NN)
            return normed_g, qkv_g, outbias_g

        def attention_weights(branch, normed_in, mix, qkv_g):
            sums = jnp.sum(qkv_g.astype(F32), axis=0).reshape(3, width)
            out_g = dot(mix, branch, TN).astype(BF16)
            in_g = dot(qkv_g, normed_in, TN).astype(BF16)
            pack = jnp.concatenate(
                [
                    in_g.reshape(3, tp, dp, hp, width)
                    .transpose(2, 1, 0, 3, 4)
                    .reshape(dp * tp, 3 * hp, width),
                    out_g.reshape(tp, dp, hp, width)
                    .transpose(1, 0, 2, 3)
                    .reshape(dp * tp, hp, width),
                ],
                axis=1,
            )
            return pack, sums

        time_branch = after_time_g.astype(BF16)
        time_in_g, time_qkv_g, time_outbias_g = attention_back(
            time_branch, time_in, time_qkv, time_mix, time_in_w, time_out_w, True
        )
        time_gain_g = jnp.sum(time_in_g * tn_p, axis=0)
        time_shift_g = jnp.sum(time_in_g, axis=0)
        after_space_g_p = after_time_g + norm_back(time_in_g, tn_p, tr_p, time_gain)

        high = exchange(after_space_g_p.astype(BF16))
        time_pack, time_sums = attention_weights(time_branch, time_in, time_mix, time_qkv_g)
        high, time_pack, time_sums, layer_out = lax.optimization_barrier(
            (high, time_pack, time_sums, layer_out)
        )
        after_space_g = high.astype(F32)

        space_in_g, space_qkv_g, space_outbias_g = attention_back(
            high, space_in, space_qkv, space_mix, space_in_w, space_out_w, False
        )
        space_pack, space_sums = attention_weights(high, space_in, space_mix, space_qkv_g)
        space_gain_g = jnp.sum(space_in_g * space_n, axis=0)
        space_shift_g = jnp.sum(space_in_g, axis=0)
        input_g = unpad(after_space_g + norm_back(space_in_g, space_n, space_r, space_gain))

        shared = jnp.concatenate(
            [
                space_gain_g, space_shift_g, space_outbias_g, time_gain_g, time_shift_g,
                time_outbias_g, feed_gain_g, feed_shift_g, down_bias_g,
            ]
        )
        headed = jnp.stack([space_sums[0], space_sums[2], time_sums[0], time_sums[2]])
        headed = headed.reshape(4, tp, heads_width).transpose(1, 0, 2).reshape(tp, -1)
        upped = up_bias_g.reshape(dp, tp, up).transpose(1, 0, 2).reshape(tp, -1)
        sharded = jnp.concatenate([headed, upped], axis=1)
        many, few = 9 * width // dp, sharded.shape[1] // dp
        small = jnp.concatenate(
            [
                jnp.broadcast_to(shared.reshape(dp, 1, many), (dp, tp, many)),
                sharded.reshape(tp, dp, few).transpose(1, 0, 2),
                jnp.zeros((dp, tp, 2 * width - many - few), F32),
            ],
            axis=2,
        ).astype(BF16)
        small = jnp.pad(small.reshape(dp * tp, 2, width), ((0, 0), (0, 14), (0, 0)))
        space_pack = jnp.concatenate([space_pack, small], axis=1)

        def spread(part):
            return lax.all_gather(part, names["dp"], axis=0, tiled=False)

        feed_part, space_pack = lax.optimization_barrier((feed_part, space_pack))
        if direct:
            time_all, space_all = scatter_sum(
                [x.reshape((dp, tp, -1, width)) for x in (time_pack, space_pack)]
            )
        else:
            both = spread(scatter(jnp.concatenate([time_pack, space_pack], axis=1)))
            time_all, space_all = both[:, : 4 * hp], both[:, 4 * hp :]

        def attn_out(full):
            in_out = full[:, : 3 * hp].reshape(dp, 3, hp, width).transpose(1, 0, 2, 3)
            in_out = in_out.reshape(3, heads_width, width).transpose(2, 0, 1).astype(F32)
            return in_out, full[:, 3 * hp : 4 * hp].reshape(heads_width, width).astype(F32)

        feed_all = spread(feed_part)
        time_in_out, time_out_out = attn_out(time_all)
        space_in_out, space_out_out = attn_out(space_all)
        sums = space_all[:, 4 * hp : 4 * hp + 2].reshape(dp, 2 * width).astype(F32)
        rows = sums[:, :many].reshape(9, width)
        own_sums = sums[:, many : many + few].reshape(-1)
        head_rows = own_sums[: 4 * heads_width].reshape(4, heads_width)
        up_bias_out = own_sums[4 * heads_width :]
        return (
            layer_out,
            input_g,
            rows[0], rows[1], space_in_out, head_rows[0:2], space_out_out, rows[2],
            rows[3], rows[4], time_in_out, head_rows[2:4], time_out_out, rows[5],
            rows[6], rows[7],
            feed_all[:, :up].reshape(units, width).astype(F32),
            up_bias_out,
            feed_all[:, up:].reshape(units, width).astype(F32),
            rows[8],
        )

    return per_device


def solution(mesh):
    inner, names, dp, tp = build(mesh)
    every, tensor = ("a", "b", "c"), names["tensor"]
    frames = P(every, None, None)
    head_in = P(None, None, tensor)
    head_bias = P(None, tensor)
    row = P(tensor, None)
    return jax.shard_map(
        make_device(names, dp, tp),
        mesh=inner,
        in_specs=(
            frames, P(), P(), head_in, head_bias, row, P(),
            P(), P(), head_in, head_bias, row, P(),
            P(), P(), row, P(tensor), row, P(), frames,
        ),
        out_specs=(
            frames, frames, P(), P(), head_in, head_bias, row, P(),
            P(), P(), head_in, head_bias, row, P(),
            P(), P(), row, P(tensor), row, P(),
        ),
        check_vma=False,
    )
```
